32 devices in a mesh: groups: 2 (over y), seq: 4 (over z), blk: 2 (over x), tp: 2 (over core).
Axes of the slice: x: 2, y: 2, z: 4, core: 2. Of those that a mesh axis runs over, the one named last changes fastest.
Arguments:
- queries: bfloat16 [2048, 8192], P(('groups', 'seq', 'blk'), 'tp'), parts along dimension 0, may hold values from -160 to 160
- rotated_keys: bfloat16 [2048, 1024], P(('groups', 'seq', 'blk'), 'tp'), parts along dimension 0, may hold values from -5 to 5
- head_value_rows: bfloat16 [2048, 1024], P(('groups', 'seq', 'blk'), 'tp'), parts along dimension 0, may hold values from -6 to 6
- doc_lengths: int32 [16], P('groups'), parts along dimension 0, may hold values from 1 to 256, 1024 in all
- owner_plan: int32 [8, 2], P('groups'), parts along dimension 0, may hold values from 0 to 3, as said below
Outputs:
- attended: bfloat16 [4096, 8192], P(('groups', 'seq', 'blk'), 'tp'), parts along dimension 0
The draws below stay inside these ranges and needn't reach their ends.
There are 2 independent parts, one for each index of `groups`. The reference program is written for one: setup_inputs(seed, part) draws one part's arguments, and reference() takes and returns one part's arrays. A program takes and returns all parts, laid end to end along the dimension named above; each array names one. Nothing has to cross between parts.
Inputs may be any that keep to these rules, and one draw needn't show every extreme that they name: `doc_lengths`: the lengths sum to 1024. `owner_plan`: group g consists of tokens g * 256 to g * 256 + 255, its block j of tokens j * 128 to j * 128 + 127 within the group. The entries of one row are distinct, so one group sends at most 1 block to one owner; in every draw some owner receives 1 block from every group.
All inputs are finite; a program needn't handle non-finite values.
Results may differ from the reference program's by a relative error of at most 0.0037.
Values may be sent and summed in bfloat16 or wider, within the bound.
No kernel may reach another device: no remote copies, remote signals or barrier semaphores. Data moves between devices by JAX's collectives and lax.ppermute only.
A program may use at most 64 MiB of HBM per device.

```python
import math
import jax
import jax.numpy as jnp
import numpy as np
from jax import lax

QUERY_HEADS = 64
KEY_HEADS = 8
HEAD_WIDTH = 128
BLOCK = 128
GROUP_BLOCKS = 2
PAIR = 1
PACKED_LENGTH = 1024
SLOTS = 512
DOC_MAX = 256
NDOCS = 8
N_SEQ = 4


def draw_both(base_key):
    key_random, query_draw = jax.random.split(base_key, 2)
    key_entries = jnp.clip(jax.random.normal(key_random, (PACKED_LENGTH, KEY_HEADS, HEAD_WIDTH), jnp.float32), -5.0, 5.0)
    query_entries = jnp.clip(jax.random.normal(query_draw, (PACKED_LENGTH, QUERY_HEADS, HEAD_WIDTH), jnp.float32), -5.0, 5.0)
    return (query_entries.reshape(PACKED_LENGTH, QUERY_HEADS * HEAD_WIDTH), key_entries.reshape(PACKED_LENGTH, KEY_HEADS * HEAD_WIDTH))


def draw_queries(key, part):
    return draw_both(jax.random.fold_in(key, 11))[0].astype(jnp.bfloat16)


def draw_rotated_keys(key, part):
    return draw_both(jax.random.fold_in(key, 11))[1].astype(jnp.bfloat16)


def draw_owner_plan(key, part):
    full_draw, pick_draw, order_draw = jax.random.split(jax.random.fold_in(key, 5), 3)
    slot_total = N_SEQ * PAIR
    full_owner = jax.random.randint(full_draw, (), 0, N_SEQ)
    slot_ids = jnp.arange(slot_total, dtype=jnp.int32)
    noise_score = jax.random.randint(pick_draw, (N_SEQ, slot_total), 0, 1 << 16) * slot_total + slot_ids[None, :]
    ranking = jnp.where((slot_ids // PAIR == full_owner)[None, :], slot_ids[None, :] - slot_total, noise_score)
    picked = jnp.argsort(ranking, axis=1)[:, :GROUP_BLOCKS]
    order_score = jax.random.randint(order_draw, (N_SEQ, GROUP_BLOCKS), 0, 1 << 16) * GROUP_BLOCKS + jnp.arange(GROUP_BLOCKS, dtype=jnp.int32)[None, :]
    order_index = jnp.argsort(order_score, axis=1)
    return jnp.take_along_axis(picked, order_index, axis=1).astype(jnp.int32)


def steps_of(rng, shape, shards, low, largest):
    loudness, own = 1.0, jax.random.fold_in(rng, 6)
    for axis_at, parts in shards:
        steps = jnp.exp(jax.random.uniform(jax.random.fold_in(own, axis_at), (parts,), jnp.float32, low / len(shards), largest / len(shards)))
        loudness = loudness * jnp.repeat(steps, shape[axis_at] // parts).reshape([-1 if axis == axis_at else 1 for axis in range(len(shape))])
    return loudness


def length_profile(number_of, total, limit, lean):
    weights = [(1 << 20) // math.isqrt(standing ** lean) + 1 for standing in range(2, number_of + 1)]
    rest, holding = total - limit - (number_of - 1), [1] * (number_of - 1)
    while rest > 0:
        movable = [i for i in range(number_of - 1) if holding[i] < limit]
        pool, left = sum([weights[i] for i in movable]), rest
        for i in movable:
            extra = min(limit - holding[i], max(1, left * weights[i] // pool), rest)
            holding[i] = holding[i] + extra
            rest = rest - extra
    return np.array([limit] + holding)


def uneven_parts(stream_key, amount, total, limit, skew):
    if amount == 2:
        one = jax.random.randint(stream_key, (), max(1, total - limit), min(limit, total - 1) + 1)
        return jnp.stack([one, total - one])
    tallies = jnp.asarray(length_profile(amount, total, limit, skew), jnp.int32)
    twos = (amount - 1) // 2
    donor, receiver = tallies[1:1 + 2 * twos:2], tallies[2:2 + 2 * twos:2]
    slack = jnp.minimum(donor - 1, limit - receiver)
    passed = jax.random.randint(jax.random.fold_in(stream_key, 1), (twos,), 0, 1 << 20) % (slack + 1)
    tallies = tallies.at[1:1 + 2 * twos:2].set(donor - passed).at[2:2 + 2 * twos:2].set(receiver + passed)
    return tallies[jax.random.permutation(jax.random.fold_in(stream_key, 2), amount)]


def gaussian(rng, extent, scale, bound, pieces=(), held_as=jnp.bfloat16):
    drawn = scale * jax.random.normal(rng, extent, jnp.float32)
    if pieces:
        drawn = drawn * steps_of(rng, extent, pieces, -0.22, 0.18)
    return jnp.clip(drawn, -bound, bound).astype(held_as)


def setup_inputs(seed: int = 0, part: int = 0) -> dict:
    arg_keys = jax.random.split(jax.random.key(seed), 6)
    own_keys = jax.random.split(jax.random.fold_in(arg_keys[5], part), 6)
    return {
        "queries": draw_queries(jax.random.fold_in(jax.random.fold_in(arg_keys[5], part), 71), part),
        "rotated_keys": draw_rotated_keys(jax.random.fold_in(jax.random.fold_in(arg_keys[5], part), 71), part),
        "head_value_rows": gaussian(own_keys[2], (PACKED_LENGTH, KEY_HEADS * HEAD_WIDTH), 1.0, 6.0, ((0, 8), (1, 2))),
        "doc_lengths": uneven_parts(own_keys[3], NDOCS, PACKED_LENGTH, DOC_MAX, 1).astype(jnp.int32),
        "owner_plan": draw_owner_plan(jax.random.fold_in(jax.random.fold_in(arg_keys[5], part), 71), part),
    }


masked_score = -1e+30

def document_of(positions, doc_ends):
    return lax.optimization_barrier(jnp.sum((positions[:, None] >= doc_ends[None, :]).astype(jnp.int32), axis=1))

def reference(queries, rotated_keys, head_value_rows, doc_lengths, owner_plan):
    total_length = queries.shape[0]
    heads_per_group = QUERY_HEADS // KEY_HEADS
    doc_ends = jnp.cumsum(doc_lengths).astype(jnp.int32)
    row_block = math.gcd(total_length, 256)
    backward_reach = DOC_MAX
    window = backward_reach + row_block
    score_scale = 1.0 / math.sqrt(HEAD_WIDTH)
    query_head_rows = queries.reshape(total_length, KEY_HEADS, heads_per_group, HEAD_WIDTH)
    key_padded_rows = jnp.concatenate([jnp.zeros((backward_reach, KEY_HEADS * HEAD_WIDTH), rotated_keys.dtype), rotated_keys], axis=0).reshape(total_length + backward_reach, KEY_HEADS, HEAD_WIDTH)
    value_padded_rows = jnp.concatenate([jnp.zeros((backward_reach, KEY_HEADS * HEAD_WIDTH), head_value_rows.dtype), head_value_rows], axis=0).reshape(total_length + backward_reach, KEY_HEADS, HEAD_WIDTH)

    def one_block(block_index):
        first_row = (block_index * row_block).astype(jnp.int32)
        query_tile = lax.dynamic_slice_in_dim(query_head_rows, first_row, row_block, 0).astype(jnp.float32)
        key_tile = lax.dynamic_slice_in_dim(key_padded_rows, first_row, window, 0).astype(jnp.float32)
        value_tile = lax.dynamic_slice_in_dim(value_padded_rows, first_row, window, 0).astype(jnp.float32)
        query_pos = first_row + jnp.arange(row_block, dtype=jnp.int32)
        key_pos = first_row - backward_reach + jnp.arange(window, dtype=jnp.int32)
        same_doc = document_of(query_pos, doc_ends)[:, None] == document_of(key_pos, doc_ends)[None, :]
        allowed = same_doc & (key_pos[None, :] <= query_pos[:, None]) & (key_pos[None, :] >= 0)
        allowed = allowed[:, None, None, :]
        scores = jnp.einsum('qghd,kgd->qghk', query_tile, key_tile, precision=lax.Precision.HIGHEST) * score_scale
        scores = jnp.where(allowed, scores, masked_score)
        highest = lax.optimization_barrier(jnp.max(scores, axis=3, keepdims=True))
        exponent = jnp.where(allowed, jnp.exp(scores - highest), 0.0)
        totals = lax.optimization_barrier(jnp.sum(exponent, axis=3))
        weights = lax.optimization_barrier(exponent.astype(jnp.bfloat16)).astype(jnp.float32)
        mixed = jnp.einsum('qghk,kgd->qghd', weights, value_tile, precision=lax.Precision.HIGHEST)
        return (mixed / totals[..., None]).astype(jnp.bfloat16).reshape(row_block, QUERY_HEADS * HEAD_WIDTH)
    token_out = lax.map(one_block, jnp.arange(total_length // row_block, dtype=jnp.int32)).reshape(total_length, QUERY_HEADS * HEAD_WIDTH)
    blocks_out = token_out.reshape(N_SEQ, GROUP_BLOCKS, BLOCK, QUERY_HEADS * HEAD_WIDTH)
    owner_ids = jnp.arange(N_SEQ, dtype=jnp.int32)
    pair_ids = jnp.arange(PAIR, dtype=jnp.int32)
    wanted = owner_ids[:, None] * PAIR + pair_ids[None, :]
    matches = owner_plan[None, :, None, :] == wanted[:, None, :, None]
    slot_live = jnp.any(matches, axis=3)
    block_pick = lax.optimization_barrier(jnp.sum(jnp.where(matches, jnp.arange(GROUP_BLOCKS, dtype=jnp.int32), 0), axis=3)).astype(jnp.int32)
    group_ids = jnp.broadcast_to(owner_ids[None, :, None], block_pick.shape)
    picked = blocks_out[group_ids, block_pick]
    picked = jnp.where(slot_live[:, :, :, None, None], picked, jnp.zeros_like(picked))
    return picked.reshape(N_SEQ * SLOTS, QUERY_HEADS * HEAD_WIDTH)
```

```python
import math

import jax
import jax.numpy as jnp
from jax import lax
from jax.experimental import pallas as pl
from jax.experimental.pallas import tpu as pltpu
from jax.sharding import PartitionSpec as P

QUERY_HEADS = 64
KEY_HEADS = 8
HEAD_WIDTH = 128
BLOCK = 128


masked_score = -1e30
exponent_scale = math.log2(math.e) / math.sqrt(HEAD_WIDTH)


def owner_of(step, group, blk, seq_count, block_axis):
    per_device = seq_count // block_axis
    return (step + blk * per_device + group % per_device) % seq_count


def attend_kernel(seq_count, block_axis, pair_room, query_columns, kv_columns, kv_width, *refs):
    doc_ref, plan_ref = refs[:2]
    query_refs = refs[2 : 2 + block_axis]
    own_key, own_value = refs[2 + block_axis : 4 + block_axis]
    home_refs = refs[4 + block_axis : 3 + 2 * block_axis]
    prior_refs = refs[3 + 2 * block_axis : 3 + 3 * block_axis]
    message_refs = refs[3 + 3 * block_axis : 3 + 3 * block_axis + seq_count]
    query_all, key_all, value_all = refs[3 + 3 * block_axis + seq_count :]
    group = lax.axis_index("seq")
    blk = lax.axis_index("blk")
    group_len = block_axis * BLOCK
    window = group_len + BLOCK
    columns = query_columns[1]
    heads = columns // HEAD_WIDTH
    kv_first, kv_size = kv_columns
    per_kv = heads // (kv_size // HEAD_WIDTH)
    doc_count = doc_ref.shape[0]

    for shift in range(block_axis):
        origin = lax.rem(blk - shift + block_axis, block_axis)
        rows = pl.ds(pl.multiple_of(origin * BLOCK, BLOCK), BLOCK)
        near_rows = pl.ds(pl.multiple_of(group_len + origin * BLOCK, BLOCK), BLOCK)
        if shift == 0:
            first = pl.multiple_of(blk * query_columns[2] + query_columns[0], HEAD_WIDTH)
            query_all[rows, :] = query_refs[0][:, pl.ds(first, columns)]
            first_kv = blk * query_columns[2] // (HEAD_WIDTH * (QUERY_HEADS // KEY_HEADS))
            near = pl.ds(pl.multiple_of(first_kv * HEAD_WIDTH + kv_first, HEAD_WIDTH), kv_size)
            key_all[near_rows, :] = own_key[:, near]
            value_all[near_rows, :] = own_value[:, near]
        else:
            query_all[rows, :] = query_refs[shift][...]
            key_all[near_rows, :] = home_refs[shift - 1][:, kv_first : kv_first + kv_size]
            value_all[near_rows, :] = home_refs[shift - 1][
                :, kv_width + kv_first : kv_width + kv_first + kv_size
            ]
        key_all[rows, :] = prior_refs[shift][:, kv_first : kv_first + kv_size]
        value_all[rows, :] = prior_refs[shift][
            :, kv_width + kv_first : kv_width + kv_first + kv_size
        ]

    def attend(block, out_ref, out_row):
        first_row = group * group_len + block * BLOCK
        query_pos = first_row + lax.broadcasted_iota(jnp.int32, (BLOCK, window), 0)
        key_pos = first_row - group_len + lax.broadcasted_iota(jnp.int32, (BLOCK, window), 1)
        row_pos = first_row + lax.broadcasted_iota(jnp.int32, (BLOCK, HEAD_WIDTH), 0)

        def reach(index, carried):
            end, start = carried
            end = end + doc_ref[index]
            return end, jnp.where(row_pos >= end, end, start)

        _, start = lax.fori_loop(
            0, doc_count, reach, (jnp.int32(0), jnp.zeros((BLOCK, HEAD_WIDTH), jnp.int32))
        )
        start = jnp.concatenate([start] * (window // HEAD_WIDTH), axis=1)
        allowed = (key_pos >= start) & (key_pos <= query_pos)
        query_rows = pl.ds(pl.multiple_of(block * BLOCK, BLOCK), BLOCK)
        key_rows = pl.ds(pl.multiple_of(block * BLOCK, BLOCK), window)
        for head in range(heads):
            at = slice(head * HEAD_WIDTH, (head + 1) * HEAD_WIDTH)
            kv_at = slice((head // per_kv) * HEAD_WIDTH, (head // per_kv + 1) * HEAD_WIDTH)
            scores = lax.dot_general(
                query_all[query_rows, at],
                key_all[key_rows, kv_at],
                (((1,), (1,)), ((), ())),
                preferred_element_type=jnp.float32,
            )
            scores = jnp.where(allowed, scores, masked_score)
            top = jnp.max(scores, axis=1, keepdims=True)
            weights = jnp.exp2((scores - top) * exponent_scale)
            total = jnp.sum(weights, axis=1, keepdims=True)
            mixed = jnp.dot(
                weights.astype(jnp.bfloat16),
                value_all[key_rows, kv_at],
                preferred_element_type=jnp.float32,
            )
            out_ref[out_row : out_row + BLOCK, at] = (mixed / total).astype(jnp.bfloat16)

    for step in range(seq_count):
        owner = owner_of(step, group, blk, seq_count, block_axis)
        for pair in range(pair_room):
            chosen = jnp.int32(-1)
            for block in range(plan_ref.shape[1]):
                chosen = jnp.where(
                    plan_ref[group, block] == owner * pair_room + pair, block, chosen
                )

            @pl.when(chosen >= 0)
            def _():
                attend(chosen, message_refs[step], pair * BLOCK)

            @pl.when(chosen < 0)
            def _():
                message_refs[step][pair * BLOCK : (pair + 1) * BLOCK, :] = jnp.zeros(
                    (BLOCK, columns), jnp.bfloat16
                )


def place_kernel(at_ref, message_ref, _, out_ref):
    out_ref[...] = message_ref[...]


def per_device(queries, rotated_keys, head_value_rows, doc_lengths, owner_plan):
    block_axis = lax.axis_size("blk")
    seq_count = lax.axis_size("seq")
    group = lax.axis_index("seq")
    blk = lax.axis_index("blk")
    local_tokens = queries.shape[0]
    group_blocks = local_tokens * block_axis // BLOCK
    heads_tp = queries.shape[1] // HEAD_WIDTH
    heads_dev = heads_tp // block_axis
    heads_per_group = QUERY_HEADS // KEY_HEADS
    groups_kv = max(1, heads_dev // heads_per_group)
    dev_width = heads_dev * HEAD_WIDTH
    kv_width = groups_kv * HEAD_WIDTH
    pair_room = -(-2 * group_blocks // seq_count)
    per_owner = seq_count // block_axis
    assert local_tokens == BLOCK and seq_count % block_axis == 0

    def permute(array, target):
        pairs = []
        for z in range(seq_count):
            for x in range(block_axis):
                to = target(z, x)
                if to is not None:
                    pairs.append((z * block_axis + x, to[0] * block_axis + to[1]))
        return lax.ppermute(array, ("seq", "blk"), pairs)

    def kv_for(to):
        first = to * heads_dev // heads_per_group * HEAD_WIDTH
        return jnp.concatenate(
            [
                lax.dynamic_slice_in_dim(rotated_keys, first, kv_width, 1),
                lax.dynamic_slice_in_dim(head_value_rows, first, kv_width, 1),
            ],
            axis=1,
        )

    home, prior = [], []
    for shift in range(block_axis):
        sent = kv_for((blk + shift) % block_axis)
        if shift:
            home.append(permute(sent, lambda z, x: (z, (x + shift) % block_axis)))
        prior.append(
            permute(
                sent, lambda z, x: (z + 1, (x + shift) % block_axis) if z + 1 < seq_count else None
            )
        )

    chunk_heads = [heads_per_group] * groups_kv if heads_dev >= heads_per_group else [heads_dev]
    slot_rows = pair_room * BLOCK
    out = jnp.zeros((per_owner * slot_rows, heads_tp * HEAD_WIDTH), jnp.bfloat16)
    first_column = 0
    for chunk, heads in enumerate(chunk_heads):
        width = heads * HEAD_WIDTH
        received = []
        for shift in range(1, block_axis):
            part = lax.dynamic_slice_in_dim(
                queries, (blk + shift) % block_axis * dev_width + first_column, width, 1
            )
            received.append(permute(part, lambda z, x: (z, (x + shift) % block_axis)))
        kernel = lambda *refs, first=first_column, width=width, chunk=chunk: attend_kernel(
            seq_count,
            block_axis,
            pair_room,
            (first, width, dev_width),
            (chunk * HEAD_WIDTH, HEAD_WIDTH),
            kv_width,
            *refs,
        )
        vmem = pl.BlockSpec(memory_space=pltpu.VMEM)
        smem = pl.BlockSpec(memory_space=pltpu.SMEM)
        vector_inputs = [queries, *received, rotated_keys, head_value_rows, *home, *prior]
        window = (block_axis + 1) * BLOCK
        messages = pl.pallas_call(
            kernel,
            out_shape=[jax.ShapeDtypeStruct((slot_rows, width), jnp.bfloat16)] * seq_count,
            in_specs=[smem, smem] + [vmem] * len(vector_inputs),
            out_specs=[vmem] * seq_count,
            scratch_shapes=[
                pltpu.VMEM((block_axis * BLOCK, width), jnp.bfloat16),
                pltpu.VMEM((2 * block_axis * BLOCK, HEAD_WIDTH), jnp.bfloat16),
                pltpu.VMEM((2 * block_axis * BLOCK, HEAD_WIDTH), jnp.bfloat16),
            ],
            cost_estimate=pl.CostEstimate(
                flops=4 * group_blocks * BLOCK * window * width,
                bytes_accessed=2 * seq_count * slot_rows * width,
                transcendentals=group_blocks * BLOCK * window * heads,
            ),
            name=f"attend_{chunk}",
        )(doc_lengths, owner_plan, *vector_inputs)
        for step in range(seq_count):
            arrived = permute(
                messages[step],
                lambda z, x: (owner_of(step, z, x, seq_count, block_axis), z // per_owner),
            )
            origin = (group - step + seq_count) % seq_count
            at = jnp.array([1, 0], jnp.int32) * (origin % per_owner) + jnp.array(
                [0, 1], jnp.int32
            ) * ((origin // per_owner) * (dev_width // width) + first_column // width)
            out = pl.pallas_call(
                place_kernel,
                grid_spec=pltpu.PrefetchScalarGridSpec(
                    num_scalar_prefetch=1,
                    grid=(1,),
                    in_specs=[
                        pl.BlockSpec((slot_rows, width), lambda i, at: (0, 0)),
                        pl.BlockSpec(memory_space=pl.ANY),
                    ],
                    out_specs=pl.BlockSpec((slot_rows, width), lambda i, at: (at[0], at[1])),
                ),
                out_shape=jax.ShapeDtypeStruct(out.shape, out.dtype),
                input_output_aliases={2: 0},
                name=f"place_{chunk}_{step}",
            )(at, arrived, out)
        first_column += width
    return out


def solution(mesh):
    in_specs = (
        P(("groups", "seq", "blk"), "tp"),
        P(("groups", "seq", "blk"), "tp"),
        P(("groups", "seq", "blk"), "tp"),
        P("groups"),
        P("groups", None),
    )
    out_specs = P(("groups", "seq", "blk"), "tp")
    return jax.shard_map(
        per_device, mesh=mesh, in_specs=in_specs, out_specs=out_specs, check_vma=False
    )
```

```python
import math

import jax
import jax.numpy as jnp
from jax import lax
from jax.experimental import pallas as pl
from jax.experimental.pallas import tpu as pltpu
from jax.sharding import PartitionSpec as P


QUERY_HEADS = 64
KEY_HEADS = 8
HEAD_WIDTH = 128
BLOCK = 128
HEADS_PER_GROUP = QUERY_HEADS // KEY_HEADS


masked_score = -1e30
exponent_scale = math.log2(math.e) / math.sqrt(HEAD_WIDTH)
vmem = pl.BlockSpec(memory_space=pltpu.VMEM)
smem = pl.BlockSpec(memory_space=pltpu.SMEM)
hbm = pl.BlockSpec(memory_space=pltpu.HBM)


def owner_of(step, group, blk, seq_count, block_axis):
    per_owner = seq_count // block_axis
    return (step + blk * per_owner + group % per_owner) % seq_count


def in_hbm(array):
    return pltpu.with_memory_space_constraint(array, pltpu.HBM)


def lanes(first, size):
    return pl.ds(pl.multiple_of(first, HEAD_WIDTH), size)


def kv_first(blk, dev_width):
    return blk * dev_width // (HEAD_WIDTH * HEADS_PER_GROUP) * HEAD_WIDTH


def pack_kernel(block_axis, dev_width, kv_width, chunks, query_ref, key_ref, value_ref, *refs):
    blk = lax.axis_index("blk")
    own_ref, prior_refs = refs[0], refs[1 : 1 + block_axis]
    rest, sems = refs[1 + block_axis : -1], refs[-1]
    moves = [(query_ref.at[:, lanes(blk * dev_width, dev_width)], own_ref)]
    for shift in range(block_axis):
        to = lax.rem(blk + shift, block_axis)
        kv = lanes(kv_first(to, dev_width), kv_width)
        targets = [prior_refs[shift]]
        for chunk, (first, size) in enumerate(chunks):
            if shift:
                out_ref = rest[chunk * (block_axis - 1) + shift - 1]
                columns = lanes(to * dev_width + first * HEAD_WIDTH, size * HEAD_WIDTH)
                if chunk == 0:
                    targets.append(out_ref)
                    out_ref = out_ref.at[:, pl.ds(2 * kv_width, size * HEAD_WIDTH)]
                moves.append((query_ref.at[:, columns], out_ref))
        for target in targets:
            moves.append((key_ref.at[:, kv], target.at[:, pl.ds(0, kv_width)]))
            moves.append((value_ref.at[:, kv], target.at[:, pl.ds(kv_width, kv_width)]))
    copies = [
        pltpu.make_async_copy(source, target, sems.at[index])
        for index, (source, target) in enumerate(moves)
    ]
    for copy in copies:
        copy.start()
    for copy in copies:
        copy.wait()


def attend_kernel(seq_count, block_axis, pair_room, kv_width, chunk, *refs):
    refs = list(refs)
    take = lambda count: [refs.pop(0) for _ in range(count)]
    doc_ref, plan_ref, own_query, own_kv = take(4)
    prior_refs = take(block_axis)
    home_refs = take(block_axis - 1)
    query_refs = take(block_axis - 1) if chunk[0] else home_refs
    message_refs = take(seq_count)
    query_all, key_all, value_all = refs
    group = lax.axis_index("seq")
    blk = lax.axis_index("blk")
    group_len = block_axis * BLOCK
    window = group_len + BLOCK
    first, heads = chunk
    columns = heads * HEAD_WIDTH
    query_at = 0 if first else 2 * kv_width
    kv_low = first // HEADS_PER_GROUP
    kv_high = (first + heads - 1) // HEADS_PER_GROUP + 1
    kv_from, kv_to = kv_low * HEAD_WIDTH, kv_high * HEAD_WIDTH
    doc_count = doc_ref.shape[0]

    for shift in range(block_axis):
        origin = lax.rem(blk - shift + block_axis, block_axis)
        rows = pl.ds(pl.multiple_of(origin * BLOCK, BLOCK), BLOCK)
        near_rows = pl.ds(pl.multiple_of(group_len + origin * BLOCK, BLOCK), BLOCK)
        if shift == 0:
            query = own_query[:, first * HEAD_WIDTH : first * HEAD_WIDTH + columns]
            home = own_kv
        else:
            query = query_refs[shift - 1][:, query_at : query_at + columns]
            home = home_refs[shift - 1]
        key_all[near_rows, :] = home[:, kv_from:kv_to]
        value_all[near_rows, :] = home[:, kv_width + kv_from : kv_width + kv_to]
        for head in range(heads):
            query_all[origin, head * BLOCK : (head + 1) * BLOCK, :] = query[
                :, head * HEAD_WIDTH : (head + 1) * HEAD_WIDTH
            ]
        key_all[rows, :] = prior_refs[shift][:, kv_from:kv_to]
        value_all[rows, :] = prior_refs[shift][:, kv_width + kv_from : kv_width + kv_to]

    def attend(block, out_ref, out_row):
        first_row = group * group_len + block * BLOCK
        query_pos = first_row + lax.broadcasted_iota(jnp.int32, (BLOCK, window), 0)
        key_pos = first_row - group_len + lax.broadcasted_iota(jnp.int32, (BLOCK, window), 1)
        row_pos = first_row + lax.broadcasted_iota(jnp.int32, (BLOCK, HEAD_WIDTH), 0)

        def reach(index, carried):
            end, start = carried
            end = end + doc_ref[index]
            return end, jnp.where(row_pos >= end, end, start)

        _, start = lax.fori_loop(
            0, doc_count, reach, (jnp.int32(0), jnp.zeros((BLOCK, HEAD_WIDTH), jnp.int32))
        )
        start = jnp.concatenate([start] * (window // HEAD_WIDTH), axis=1)
        allowed = (key_pos >= start) & (key_pos <= query_pos)
        key_rows = pl.ds(pl.multiple_of(block * BLOCK, BLOCK), window)
        for kv in range(kv_low, kv_high):
            low = max(first, kv * HEADS_PER_GROUP) - first
            high = min(first + heads, (kv + 1) * HEADS_PER_GROUP) - first
            kv_at = slice((kv - kv_low) * HEAD_WIDTH, (kv - kv_low + 1) * HEAD_WIDTH)
            scores = lax.dot_general(
                query_all[block, low * BLOCK : high * BLOCK, :],
                key_all[key_rows, kv_at],
                (((1,), (1,)), ((), ())),
                preferred_element_type=jnp.float32,
            )
            weights, totals = [], []
            for head in range(high - low):
                score = scores[head * BLOCK : (head + 1) * BLOCK]
                score = jnp.where(allowed, score, masked_score)
                top = jnp.max(score, axis=1, keepdims=True)
                weight = jnp.exp2((score - top) * exponent_scale)
                totals.append(jnp.sum(weight, axis=1, keepdims=True))
                weights.append(weight.astype(jnp.bfloat16))
            mixed = jnp.dot(
                jnp.concatenate(weights, axis=0),
                value_all[key_rows, kv_at],
                preferred_element_type=jnp.float32,
            )
            for head in range(high - low):
                at = slice((low + head) * HEAD_WIDTH, (low + head + 1) * HEAD_WIDTH)
                out_ref[out_row : out_row + BLOCK, at] = (
                    mixed[head * BLOCK : (head + 1) * BLOCK] / totals[head]
                ).astype(jnp.bfloat16)

    for step in range(seq_count):
        owner = owner_of(step, group, blk, seq_count, block_axis)
        for pair in range(pair_room):
            chosen = jnp.int32(-1)
            for block in range(plan_ref.shape[0]):
                chosen = jnp.where(
                    plan_ref[block, group] == owner * pair_room + pair, block, chosen
                )

            @pl.when(chosen >= 0)
            def _():
                attend(chosen, message_refs[step], pair * BLOCK)

            @pl.when(chosen < 0)
            def _():
                message_refs[step][pair * BLOCK : (pair + 1) * BLOCK, :] = jnp.zeros(
                    (BLOCK, columns), jnp.bfloat16
                )


def place_kernel(seq_count, block_axis, dev_width, first, *refs):
    messages = refs[:seq_count]
    out_ref, sems = refs[-2:]
    group = lax.axis_index("seq")
    per_owner = seq_count // block_axis
    rows, width = messages[0].shape
    copies = []
    for step in range(seq_count):
        origin = lax.rem(group - step + seq_count, seq_count)
        at_rows = pl.ds(pl.multiple_of(lax.rem(origin, per_owner) * rows, rows), rows)
        at_lanes = lanes(origin // per_owner * dev_width + first * HEAD_WIDTH, width)
        copies.append(
            pltpu.make_async_copy(messages[step], out_ref.at[at_rows, at_lanes], sems.at[step])
        )
    for copy in copies:
        copy.start()
    for copy in copies:
        copy.wait()


def per_device(queries, rotated_keys, head_value_rows, doc_lengths, owner_plan):
    block_axis = lax.axis_size("blk")
    seq_count = lax.axis_size("seq")
    local_tokens = queries.shape[0]
    group_blocks = local_tokens * block_axis // BLOCK
    heads_tp = queries.shape[1] // HEAD_WIDTH
    heads_dev = heads_tp // block_axis
    groups_kv = max(1, heads_dev // HEADS_PER_GROUP)
    dev_width = heads_dev * HEAD_WIDTH
    kv_width = groups_kv * HEAD_WIDTH
    pair_room = -(-2 * group_blocks // seq_count)
    per_owner = seq_count // block_axis
    slot_rows = pair_room * BLOCK
    window = (block_axis + 1) * BLOCK
    assert local_tokens == BLOCK and seq_count % block_axis == 0

    def permute(array, target):
        pairs = []
        for z in range(seq_count):
            for x in range(block_axis):
                to = target(z, x)
                if to is not None:
                    pairs.append((z * block_axis + x, to[0] * block_axis + to[1]))
        return lax.ppermute(array, ("seq", "blk"), pairs)

    head_counts = [heads_dev // 4, heads_dev - heads_dev // 4]
    chunks = [(sum(head_counts[:i]), count) for i, count in enumerate(head_counts)]

    bf16 = lambda *shape: jax.ShapeDtypeStruct(shape, jnp.bfloat16)
    peers = block_axis - 1
    out_shape = [bf16(BLOCK, dev_width)] + [bf16(BLOCK, 2 * kv_width)] * block_axis
    for first, size in chunks:
        out_shape += [bf16(BLOCK, size * HEAD_WIDTH + (0 if first else 2 * kv_width))] * peers
    own_query, *packed = pl.pallas_call(
        lambda *refs: pack_kernel(block_axis, dev_width, kv_width, chunks, *refs),
        out_shape=out_shape,
        in_specs=[hbm] * 3,
        out_specs=[vmem] * len(out_shape),
        scratch_shapes=[
            pltpu.SemaphoreType.DMA((1 + 2 * block_axis + peers * (2 + len(chunks)),))
        ],
        compiler_params=pltpu.CompilerParams(vmem_limit_bytes=8 << 20),
        name="pack",
    )(*map(in_hbm, (queries, rotated_keys, head_value_rows)))

    sideways = lambda shift: lambda z, x: (z, (x + shift) % block_axis)
    onward = lambda shift: lambda z, x: (
        (z + 1, (x + shift) % block_axis) if z + 1 < seq_count else None
    )
    home = [permute(packed[block_axis + s - 1], sideways(s)) for s in range(1, block_axis)]
    prior = [permute(packed[s], onward(s)) for s in range(block_axis)]
    later = [
        [permute(packed[block_axis + c * peers + s - 1], sideways(s)) for s in range(1, block_axis)]
        for c in range(1, len(chunks))
    ]

    out = None
    for index, chunk in enumerate(chunks):
        first, heads = chunk
        width = heads * HEAD_WIDTH
        kv_span = (
            (first + heads - 1) // HEADS_PER_GROUP + 1 - first // HEADS_PER_GROUP
        ) * HEAD_WIDTH
        inputs = [own_query, packed[0], *prior, *home]
        if index:
            inputs += later[index - 1]
        attend = pl.pallas_call(
            lambda *refs, chunk=chunk: attend_kernel(
                seq_count, block_axis, pair_room, kv_width, chunk, *refs
            ),
            out_shape=[bf16(slot_rows, width)] * seq_count,
            in_specs=[smem, smem] + [vmem] * len(inputs),
            out_specs=[vmem] * seq_count,
            scratch_shapes=[
                pltpu.VMEM((block_axis, heads * BLOCK, HEAD_WIDTH), jnp.bfloat16),
                pltpu.VMEM((2 * block_axis * BLOCK, kv_span), jnp.bfloat16),
                pltpu.VMEM((2 * block_axis * BLOCK, kv_span), jnp.bfloat16),
            ],
            cost_estimate=pl.CostEstimate(
                flops=8 * group_blocks * BLOCK * window * width,
                bytes_accessed=2 * seq_count * slot_rows * width,
                transcendentals=group_blocks * BLOCK * window * heads,
            ),
            compiler_params=pltpu.CompilerParams(vmem_limit_bytes=16 << 20),
        )
        messages = attend(in_hbm(doc_lengths), in_hbm(owner_plan.T), *inputs)
        arrived = [
            permute(
                messages[step],
                lambda z, x: (owner_of(step, z, x, seq_count, block_axis), z // per_owner),
            )
            for step in range(seq_count)
        ]
        carried = [] if out is None else [out]
        out = pl.pallas_call(
            lambda *refs, first=first: place_kernel(
                seq_count, block_axis, dev_width, first, *refs
            ),
            out_shape=bf16(per_owner * slot_rows, heads_tp * HEAD_WIDTH),
            in_specs=[vmem] * seq_count + [hbm] * len(carried),
            out_specs=hbm,
            scratch_shapes=[pltpu.SemaphoreType.DMA((seq_count,))],
            input_output_aliases={seq_count: 0} if carried else {},
            compiler_params=pltpu.CompilerParams(vmem_limit_bytes=8 << 20),
        )(*arrived, *carried)
    return out


def solution(mesh):
    in_specs = (
        P(("groups", "seq", "blk"), "tp"),
        P(("groups", "seq", "blk"), "tp"),
        P(("groups", "seq", "blk"), "tp"),
        P("groups"),
        P("groups", None),
    )
    out_specs = P(("groups", "seq", "blk"), "tp")

    return jax.shard_map(
        per_device, mesh=mesh, in_specs=in_specs, out_specs=out_specs, check_vma=False
    )
```

```python
import math

import jax
import jax.numpy as jnp
from jax import lax
from jax.experimental import pallas as pl
from jax.experimental.pallas import tpu as pltpu
from jax.sharding import PartitionSpec as P


QUERY_HEADS = 64
KEY_HEADS = 8
HEAD_WIDTH = 128
BLOCK = 128
HEADS_PER_GROUP = QUERY_HEADS // KEY_HEADS


masked_score = -1e30
exponent_scale = math.log2(math.e) / math.sqrt(HEAD_WIDTH)
vmem = pl.BlockSpec(memory_space=pltpu.VMEM)
smem = pl.BlockSpec(memory_space=pltpu.SMEM)
hbm = pl.BlockSpec(memory_space=pltpu.HBM)


def owner_of(step, group, blk, seq_count, block_axis):
    return group ^ step ^ (blk * (seq_count // block_axis))


def in_hbm(array):
    return pltpu.with_memory_space_constraint(array, pltpu.HBM)


def lanes(first, size):
    return pl.ds(pl.multiple_of(first, HEAD_WIDTH), size)


def kv_first(blk, dev_width):
    return blk * dev_width // (HEAD_WIDTH * HEADS_PER_GROUP) * HEAD_WIDTH


def pack_kernel(block_axis, dev_width, kv_width, chunks, query_ref, key_ref, value_ref, *refs):
    blk = lax.axis_index("blk")
    own_ref, prior_refs = refs[0], refs[1 : 1 + block_axis]
    rest, sems = refs[1 + block_axis : -1], refs[-1]
    moves = [(query_ref.at[:, lanes(blk * dev_width, dev_width)], own_ref)]
    for shift in range(block_axis):
        to = lax.rem(blk + shift, block_axis)
        kv = lanes(kv_first(to, dev_width), kv_width)
        targets = [prior_refs[shift]]
        for chunk, (first, size) in enumerate(chunks):
            if shift:
                out_ref = rest[chunk * (block_axis - 1) + shift - 1]
                columns = lanes(to * dev_width + first * HEAD_WIDTH, size * HEAD_WIDTH)
                if chunk == 0:
                    targets.append(out_ref)
                    out_ref = out_ref.at[:, pl.ds(2 * kv_width, size * HEAD_WIDTH)]
                moves.append((query_ref.at[:, columns], out_ref))
        for target in targets:
            moves.append((key_ref.at[:, kv], target.at[:, pl.ds(0, kv_width)]))
            moves.append((value_ref.at[:, kv], target.at[:, pl.ds(kv_width, kv_width)]))
    copies = [
        pltpu.make_async_copy(source, target, sems.at[index])
        for index, (source, target) in enumerate(moves)
    ]
    for copy in copies:
        copy.start()
    for copy in copies:
        copy.wait()


def attend_kernel(seq_count, block_axis, pair_room, kv_width, chunk, *refs):
    refs = list(refs)
    take = lambda count: [refs.pop(0) for _ in range(count)]
    doc_ref, plan_ref, own_query, own_kv = take(4)
    prior_refs = take(block_axis)
    home_refs = take(block_axis - 1)
    query_refs = take(block_axis - 1) if chunk[0] else home_refs
    message_refs = take(seq_count)
    query_all, key_all, value_all = refs
    group = lax.axis_index("seq")
    blk = lax.axis_index("blk")
    group_len = block_axis * BLOCK
    window = group_len + BLOCK
    first, heads = chunk
    columns = heads * HEAD_WIDTH
    query_at = 0 if first else 2 * kv_width
    kv_low = first // HEADS_PER_GROUP
    kv_high = (first + heads - 1) // HEADS_PER_GROUP + 1
    kv_from, kv_to = kv_low * HEAD_WIDTH, kv_high * HEAD_WIDTH
    doc_count = doc_ref.shape[0]

    for shift in range(block_axis):
        origin = lax.rem(blk - shift + block_axis, block_axis)
        rows = pl.ds(pl.multiple_of(origin * BLOCK, BLOCK), BLOCK)
        near_rows = pl.ds(pl.multiple_of(group_len + origin * BLOCK, BLOCK), BLOCK)
        if shift == 0:
            query = own_query[:, first * HEAD_WIDTH : first * HEAD_WIDTH + columns]
            home = own_kv
        else:
            query = query_refs[shift - 1][:, query_at : query_at + columns]
            home = home_refs[shift - 1]
        key_all[near_rows, :] = home[:, kv_from:kv_to]
        value_all[near_rows, :] = home[:, kv_width + kv_from : kv_width + kv_to]
        for head in range(heads):
            query_all[origin, head * BLOCK : (head + 1) * BLOCK, :] = query[
                :, head * HEAD_WIDTH : (head + 1) * HEAD_WIDTH
            ]
        key_all[rows, :] = prior_refs[shift][:, kv_from:kv_to]
        value_all[rows, :] = prior_refs[shift][:, kv_width + kv_from : kv_width + kv_to]

    def attend(block, out_ref, out_row):
        first_row = group * group_len + block * BLOCK
        query_pos = first_row + lax.broadcasted_iota(jnp.int32, (BLOCK, window), 0)
        key_pos = first_row - group_len + lax.broadcasted_iota(jnp.int32, (BLOCK, window), 1)
        row_pos = first_row + lax.broadcasted_iota(jnp.int32, (BLOCK, HEAD_WIDTH), 0)

        def reach(index, carried):
            end, start = carried
            end = end + doc_ref[index]
            return end, jnp.where(row_pos >= end, end, start)

        _, start = lax.fori_loop(
            0, doc_count, reach, (jnp.int32(0), jnp.zeros((BLOCK, HEAD_WIDTH), jnp.int32))
        )
        start = jnp.concatenate([start] * (window // HEAD_WIDTH), axis=1)
        allowed = (key_pos >= start) & (key_pos <= query_pos)
        key_rows = pl.ds(pl.multiple_of(block * BLOCK, BLOCK), window)
        for kv in range(kv_low, kv_high):
            low = max(first, kv * HEADS_PER_GROUP) - first
            high = min(first + heads, (kv + 1) * HEADS_PER_GROUP) - first
            kv_at = slice((kv - kv_low) * HEAD_WIDTH, (kv - kv_low + 1) * HEAD_WIDTH)
            scores = lax.dot_general(
                query_all[block, low * BLOCK : high * BLOCK, :],
                key_all[key_rows, kv_at],
                (((1,), (1,)), ((), ())),
                preferred_element_type=jnp.float32,
            )
            weights, totals = [], []
            for head in range(high - low):
                score = scores[head * BLOCK : (head + 1) * BLOCK]
                score = jnp.where(allowed, score, masked_score)
                top = jnp.max(score, axis=1, keepdims=True)
                weight = jnp.exp2((score - top) * exponent_scale)
                totals.append(jnp.sum(weight, axis=1, keepdims=True))
                weights.append(weight.astype(jnp.bfloat16))
            mixed = jnp.dot(
                jnp.concatenate(weights, axis=0),
                value_all[key_rows, kv_at],
                preferred_element_type=jnp.float32,
            )
            for head in range(high - low):
                at = slice((low + head) * HEAD_WIDTH, (low + head + 1) * HEAD_WIDTH)
                out_ref[out_row : out_row + BLOCK, at] = (
                    mixed[head * BLOCK : (head + 1) * BLOCK] / totals[head]
                ).astype(jnp.bfloat16)

    for step in range(seq_count):
        owner = owner_of(step, group, blk, seq_count, block_axis)
        for pair in range(pair_room):
            chosen = jnp.int32(-1)
            for block in range(plan_ref.shape[0]):
                chosen = jnp.where(
                    plan_ref[block, group] == owner * pair_room + pair, block, chosen
                )

            @pl.when(chosen >= 0)
            def _():
                attend(chosen, message_refs[step], pair * BLOCK)

            @pl.when(chosen < 0)
            def _():
                message_refs[step][pair * BLOCK : (pair + 1) * BLOCK, :] = jnp.zeros(
                    (BLOCK, columns), jnp.bfloat16
                )


def place_kernel(seq_count, block_axis, dev_width, first, *refs):
    messages = refs[:seq_count]
    out_ref, sems = refs[-2:]
    group = lax.axis_index("seq")
    blk = lax.axis_index("blk")
    per_owner = seq_count // block_axis
    rows, width = messages[0].shape
    copies = []
    for step in range(seq_count):
        origin = group ^ step ^ (blk * per_owner)
        at_rows = pl.ds(pl.multiple_of(lax.rem(origin, per_owner) * rows, rows), rows)
        at_lanes = lanes(origin // per_owner * dev_width + first * HEAD_WIDTH, width)
        copies.append(
            pltpu.make_async_copy(messages[step], out_ref.at[at_rows, at_lanes], sems.at[step])
        )
    for copy in copies:
        copy.start()
    for copy in copies:
        copy.wait()


def per_device(queries, rotated_keys, head_value_rows, doc_lengths, owner_plan):
    block_axis = lax.axis_size("blk")
    seq_count = lax.axis_size("seq")
    local_tokens = queries.shape[0]
    group_blocks = local_tokens * block_axis // BLOCK
    heads_tp = queries.shape[1] // HEAD_WIDTH
    heads_dev = heads_tp // block_axis
    groups_kv = max(1, heads_dev // HEADS_PER_GROUP)
    dev_width = heads_dev * HEAD_WIDTH
    kv_width = groups_kv * HEAD_WIDTH
    pair_room = -(-2 * group_blocks // seq_count)
    per_owner = seq_count // block_axis
    slot_rows = pair_room * BLOCK
    window = (block_axis + 1) * BLOCK
    assert local_tokens == BLOCK and seq_count % block_axis == 0
    assert seq_count & (seq_count - 1) == 0 and block_axis & (block_axis - 1) == 0

    def permute(array, target):
        pairs = []
        for z in range(seq_count):
            for x in range(block_axis):
                to = target(z, x)
                pairs.append((z * block_axis + x, to[0] * block_axis + to[1]))
        return lax.ppermute(array, ("seq", "blk"), pairs)

    head_counts = [heads_dev // 4, heads_dev - heads_dev // 4]
    chunks = [(sum(head_counts[:i]), count) for i, count in enumerate(head_counts)]

    bf16 = lambda *shape: jax.ShapeDtypeStruct(shape, jnp.bfloat16)
    peers = block_axis - 1
    out_shape = [bf16(BLOCK, dev_width)] + [bf16(BLOCK, 2 * kv_width)] * block_axis
    for first, size in chunks:
        out_shape += [bf16(BLOCK, size * HEAD_WIDTH + (0 if first else 2 * kv_width))] * peers
    own_query, *packed = pl.pallas_call(
        lambda *refs: pack_kernel(block_axis, dev_width, kv_width, chunks, *refs),
        out_shape=out_shape,
        in_specs=[hbm] * 3,
        out_specs=[vmem] * len(out_shape),
        scratch_shapes=[
            pltpu.SemaphoreType.DMA((1 + 2 * block_axis + peers * (2 + len(chunks)),))
        ],
        compiler_params=pltpu.CompilerParams(vmem_limit_bytes=8 << 20),
        name="pack",
    )(*map(in_hbm, (queries, rotated_keys, head_value_rows)))

    sideways = lambda shift: lambda z, x: (z, (x + shift) % block_axis)
    onward = lambda shift: lambda z, x: ((z + 1) % seq_count, (x + shift) % block_axis)
    home = [permute(packed[block_axis + s - 1], sideways(s)) for s in range(1, block_axis)]
    prior = [permute(packed[s], onward(s)) for s in range(block_axis)]
    later = [
        [permute(packed[block_axis + c * peers + s - 1], sideways(s)) for s in range(1, block_axis)]
        for c in range(1, len(chunks))
    ]

    out = None
    for index, chunk in enumerate(chunks):
        first, heads = chunk
        width = heads * HEAD_WIDTH
        kv_span = (
            (first + heads - 1) // HEADS_PER_GROUP + 1 - first // HEADS_PER_GROUP
        ) * HEAD_WIDTH
        inputs = [own_query, packed[0], *prior, *home]
        if index:
            inputs += later[index - 1]
        attend = pl.pallas_call(
            lambda *refs, chunk=chunk: attend_kernel(
                seq_count, block_axis, pair_room, kv_width, chunk, *refs
            ),
            out_shape=[bf16(slot_rows, width)] * seq_count,
            in_specs=[smem, smem] + [vmem] * len(inputs),
            out_specs=[vmem] * seq_count,
            scratch_shapes=[
                pltpu.VMEM((block_axis, heads * BLOCK, HEAD_WIDTH), jnp.bfloat16),
                pltpu.VMEM((2 * block_axis * BLOCK, kv_span), jnp.bfloat16),
                pltpu.VMEM((2 * block_axis * BLOCK, kv_span), jnp.bfloat16),
            ],
            cost_estimate=pl.CostEstimate(
                flops=8 * group_blocks * BLOCK * window * width,
                bytes_accessed=2 * seq_count * slot_rows * width,
                transcendentals=group_blocks * BLOCK * window * heads,
            ),
            compiler_params=pltpu.CompilerParams(vmem_limit_bytes=16 << 20),
        )
        messages = attend(in_hbm(doc_lengths), in_hbm(owner_plan.T), *inputs)
        arrived = [
            permute(
                messages[step],
                lambda z, x: (owner_of(step, z, x, seq_count, block_axis), z // per_owner),
            )
            for step in range(seq_count)
        ]
        carried = [] if out is None else [out]
        out = pl.pallas_call(
            lambda *refs, first=first: place_kernel(
                seq_count, block_axis, dev_width, first, *refs
            ),
            out_shape=bf16(per_owner * slot_rows, heads_tp * HEAD_WIDTH),
            in_specs=[vmem] * seq_count + [hbm] * len(carried),
            out_specs=hbm,
            scratch_shapes=[pltpu.SemaphoreType.DMA((seq_count,))],
            input_output_aliases={seq_count: 0} if carried else {},
            compiler_params=pltpu.CompilerParams(vmem_limit_bytes=8 << 20),
        )(*arrived, *carried)
    return out


def solution(mesh):
    in_specs = (
        P(("groups", "seq", "blk"), "tp"),
        P(("groups", "seq", "blk"), "tp"),
        P(("groups", "seq", "blk"), "tp"),
        P("groups"),
        P("groups", None),
    )
    out_specs = P(("groups", "seq", "blk"), "tp")

    return jax.shard_map(
        per_device, mesh=mesh, in_specs=in_specs, out_specs=out_specs, check_vma=False
    )
```

```python
import math

import jax
import jax.numpy as jnp
from jax import lax
from jax.experimental import pallas as pl
from jax.experimental.pallas import tpu as pltpu
from jax.sharding import PartitionSpec as P


QUERY_HEADS = 64
KEY_HEADS = 8
HEAD_WIDTH = 128
BLOCK = 128
HEADS_PER_GROUP = QUERY_HEADS // KEY_HEADS


masked_score = -1e30
exponent_scale = math.log2(math.e) / math.sqrt(HEAD_WIDTH)
vmem = pl.BlockSpec(memory_space=pltpu.VMEM)
smem = pl.BlockSpec(memory_space=pltpu.SMEM)
anywhere = pl.BlockSpec(memory_space=pl.ANY)
hbm = pl.BlockSpec(memory_space=pltpu.HBM)


def owner_of(step, group, blk, seq_count, block_axis):
    per_owner = seq_count // block_axis
    return (step + blk * per_owner + group % per_owner) % seq_count


def in_hbm(array):
    return pltpu.with_memory_space_constraint(array, pltpu.HBM)


def lanes(first, size):
    return pl.ds(pl.multiple_of(first, HEAD_WIDTH), size)


def kv_first(blk, dev_width):
    return blk * dev_width // (HEAD_WIDTH * HEADS_PER_GROUP) * HEAD_WIDTH


def kv_range(chunk):
    first, heads = chunk
    return first // HEADS_PER_GROUP, (first + heads - 1) // HEADS_PER_GROUP + 1


def new_kv(chunks, index):
    seen = kv_range(chunks[index - 1])[1] if index else 0
    return seen, kv_range(chunks[index])[1]


def cut_choices(seq_count):
    if seq_count != 4:
        return []
    half = seq_count // 2
    low, high = range(half), range(half, seq_count)
    up = [(group, owner) for group in low for owner in high]
    down = [(group, owner) for group in high for owner in low]
    return [(u, d) for u in up[:2] for d in down[2:]] + [(u, d) for u in up[2:] for d in down[:2]]


def is_empty(plan_ref, pair_room, pair):
    group, owner = pair
    empty = jnp.bool_(True)
    for block in range(plan_ref.shape[0]):
        slot = plan_ref[block, group]
        empty = empty & ((slot < owner * pair_room) | (slot >= (owner + 1) * pair_room))
    return empty


def pack_kernel(block_axis, dev_width, kv_width, chunks, query_ref, key_ref, value_ref, *refs):
    blk = lax.axis_index("blk")
    own_ref, prior_refs = refs[0], refs[1 : 1 + block_axis]
    rest, sems = refs[1 + block_axis : -1], refs[-1]
    moves = [(query_ref.at[:, lanes(blk * dev_width, dev_width)], own_ref)]
    for shift in range(block_axis):
        to = lax.rem(blk + shift, block_axis)
        base = kv_first(to, dev_width)
        kv = lanes(base, kv_width)
        moves.append((key_ref.at[:, kv], prior_refs[shift].at[:, pl.ds(0, kv_width)]))
        moves.append((value_ref.at[:, kv], prior_refs[shift].at[:, pl.ds(kv_width, kv_width)]))
        if shift == 0:
            continue
        for chunk, (first, size) in enumerate(chunks):
            out_ref = rest[chunk * (block_axis - 1) + shift - 1]
            low, high = new_kv(chunks, chunk)
            span = (high - low) * HEAD_WIDTH
            if span:
                kv = lanes(base + low * HEAD_WIDTH, span)
                moves.append((key_ref.at[:, kv], out_ref.at[:, pl.ds(0, span)]))
                moves.append((value_ref.at[:, kv], out_ref.at[:, pl.ds(span, span)]))
            columns = lanes(to * dev_width + first * HEAD_WIDTH, size * HEAD_WIDTH)
            moves.append(
                (query_ref.at[:, columns], out_ref.at[:, pl.ds(2 * span, size * HEAD_WIDTH)])
            )
    copies = [
        pltpu.make_async_copy(source, target, sems.at[index])
        for index, (source, target) in enumerate(moves)
    ]
    for copy in copies:
        copy.start()
    for copy in copies:
        copy.wait()


def attend_kernel(seq_count, block_axis, pair_room, kv_width, chunks, cuts, index, *refs):
    refs = list(refs)
    take = lambda count: [refs.pop(0) for _ in range(count)]
    doc_ref, plan_ref, own_query, own_kv = take(4)
    prior_refs = take(block_axis)
    home_refs = [take(block_axis - 1) for _ in range(index + 1)]
    message_refs = take(seq_count)
    if index == 0:
        (choice_ref,) = take(1)
        empty = {}
        for pair in sum(cuts, ()):
            empty[pair] = is_empty(plan_ref, pair_room, pair)
        choice = jnp.int32(len(cuts))
        for number, (up, down) in reversed(list(enumerate(cuts))):
            choice = jnp.where(empty[up] & empty[down], number, choice)
        choice_ref[0] = choice
    query_all, key_all, value_all = refs
    group = lax.axis_index("seq")
    blk = lax.axis_index("blk")
    group_len = block_axis * BLOCK
    window = group_len + BLOCK
    first, heads = chunks[index]
    columns = heads * HEAD_WIDTH
    kv_low, kv_high = kv_range(chunks[index])
    kv_from, kv_to = kv_low * HEAD_WIDTH, kv_high * HEAD_WIDTH
    new_low, new_high = new_kv(chunks, index)
    query_at = 2 * (new_high - new_low) * HEAD_WIDTH
    doc_count = doc_ref.shape[0]

    for shift in range(block_axis):
        origin = lax.rem(blk - shift + block_axis, block_axis)
        rows = pl.ds(pl.multiple_of(origin * BLOCK, BLOCK), BLOCK)
        near_rows = pl.ds(pl.multiple_of(group_len + origin * BLOCK, BLOCK), BLOCK)
        if shift == 0:
            query = own_query[:, first * HEAD_WIDTH : first * HEAD_WIDTH + columns]
            key_all[near_rows, :] = own_kv[:, kv_from:kv_to]
            value_all[near_rows, :] = own_kv[:, kv_width + kv_from : kv_width + kv_to]
        else:
            query = home_refs[index][shift - 1][:, query_at : query_at + columns]
            for came in range(index + 1):
                low, high = new_kv(chunks, came)
                span = (high - low) * HEAD_WIDTH
                skip = max(kv_low - low, 0) * HEAD_WIDTH
                if skip >= span:
                    continue
                to = slice((low - kv_low) * HEAD_WIDTH + skip, (high - kv_low) * HEAD_WIDTH)
                home = home_refs[came][shift - 1]
                key_all[near_rows, to] = home[:, skip:span]
                value_all[near_rows, to] = home[:, span + skip : 2 * span]
        for head in range(heads):
            query_all[origin, head * BLOCK : (head + 1) * BLOCK, :] = query[
                :, head * HEAD_WIDTH : (head + 1) * HEAD_WIDTH
            ]
        key_all[rows, :] = prior_refs[shift][:, kv_from:kv_to]
        value_all[rows, :] = prior_refs[shift][:, kv_width + kv_from : kv_width + kv_to]

    def attend(block, out_ref, out_row):
        first_row = group * group_len + block * BLOCK
        query_pos = first_row + lax.broadcasted_iota(jnp.int32, (BLOCK, window), 0)
        key_pos = first_row - group_len + lax.broadcasted_iota(jnp.int32, (BLOCK, window), 1)
        row_pos = first_row + lax.broadcasted_iota(jnp.int32, (BLOCK, HEAD_WIDTH), 0)

        def reach(index, carried):
            end, start = carried
            end = end + doc_ref[index]
            return end, jnp.where(row_pos >= end, end, start)

        _, start = lax.fori_loop(
            0, doc_count, reach, (jnp.int32(0), jnp.zeros((BLOCK, HEAD_WIDTH), jnp.int32))
        )
        start = jnp.concatenate([start] * (window // HEAD_WIDTH), axis=1)
        allowed = (key_pos >= start) & (key_pos <= query_pos)
        key_rows = pl.ds(pl.multiple_of(block * BLOCK, BLOCK), window)
        for kv in range(kv_low, kv_high):
            low = max(first, kv * HEADS_PER_GROUP) - first
            high = min(first + heads, (kv + 1) * HEADS_PER_GROUP) - first
            kv_at = slice((kv - kv_low) * HEAD_WIDTH, (kv - kv_low + 1) * HEAD_WIDTH)
            scores = lax.dot_general(
                query_all[block, low * BLOCK : high * BLOCK, :],
                key_all[key_rows, kv_at],
                (((1,), (1,)), ((), ())),
                preferred_element_type=jnp.float32,
            )
            weights, totals = [], []
            for head in range(high - low):
                score = scores[head * BLOCK : (head + 1) * BLOCK]
                score = jnp.where(allowed, score, masked_score)
                top = jnp.max(score, axis=1, keepdims=True)
                weight = jnp.exp2((score - top) * exponent_scale)
                totals.append(jnp.sum(weight, axis=1, keepdims=True))
                weights.append(weight.astype(jnp.bfloat16))
            mixed = jnp.dot(
                jnp.concatenate(weights, axis=0),
                value_all[key_rows, kv_at],
                preferred_element_type=jnp.float32,
            )
            for head in range(high - low):
                at = slice((low + head) * HEAD_WIDTH, (low + head + 1) * HEAD_WIDTH)
                out_ref[out_row : out_row + BLOCK, at] = (
                    mixed[head * BLOCK : (head + 1) * BLOCK] / totals[head]
                ).astype(jnp.bfloat16)

    for step in range(seq_count):
        owner = owner_of(step, group, blk, seq_count, block_axis)
        for pair in range(pair_room):
            chosen = jnp.int32(-1)
            for block in range(plan_ref.shape[0]):
                chosen = jnp.where(
                    plan_ref[block, group] == owner * pair_room + pair, block, chosen
                )

            @pl.when(chosen >= 0)
            def _():
                attend(chosen, message_refs[step], pair * BLOCK)

            @pl.when(chosen < 0)
            def _():
                message_refs[step][pair * BLOCK : (pair + 1) * BLOCK, :] = jnp.zeros(
                    (BLOCK, columns), jnp.bfloat16
                )


def place_kernel(seq_count, block_axis, dev_width, first, *refs):
    messages = refs[:seq_count]
    out_ref, sems = refs[-2:]
    group = lax.axis_index("seq")
    per_owner = seq_count // block_axis
    rows, width = messages[0].shape
    copies = []
    for step, message_ref in enumerate(messages):
        origin = lax.rem(group - step + seq_count, seq_count)
        at_rows = pl.ds(pl.multiple_of(lax.rem(origin, per_owner) * rows, rows), rows)
        at_lanes = lanes(origin // per_owner * dev_width + first * HEAD_WIDTH, width)
        copies.append(
            pltpu.make_async_copy(message_ref, out_ref.at[at_rows, at_lanes], sems.at[step])
        )
    for copy in copies:
        copy.start()
    for copy in copies:
        copy.wait()


def per_device(queries, rotated_keys, head_value_rows, doc_lengths, owner_plan):
    block_axis = lax.axis_size("blk")
    seq_count = lax.axis_size("seq")
    local_tokens = queries.shape[0]
    group_blocks = local_tokens * block_axis // BLOCK
    heads_tp = queries.shape[1] // HEAD_WIDTH
    heads_dev = heads_tp // block_axis
    groups_kv = max(1, heads_dev // HEADS_PER_GROUP)
    dev_width = heads_dev * HEAD_WIDTH
    kv_width = groups_kv * HEAD_WIDTH
    pair_room = -(-2 * group_blocks // seq_count)
    per_owner = seq_count // block_axis
    slot_rows = pair_room * BLOCK
    window = (block_axis + 1) * BLOCK
    assert local_tokens == BLOCK and seq_count % block_axis == 0

    def permute(array, target):
        pairs = []
        for z in range(seq_count):
            for x in range(block_axis):
                to = target(z, x)
                if to is not None:
                    pairs.append((z * block_axis + x, to[0] * block_axis + to[1]))
        return lax.ppermute(array, ("seq", "blk"), pairs)

    head_counts = [heads_dev // 4, heads_dev - heads_dev // 4]
    chunks = [(sum(head_counts[:i]), count) for i, count in enumerate(head_counts)]

    bf16 = lambda *shape: jax.ShapeDtypeStruct(shape, jnp.bfloat16)
    peers = block_axis - 1
    out_shape = [bf16(BLOCK, dev_width)] + [bf16(BLOCK, 2 * kv_width)] * block_axis
    for index, (first, size) in enumerate(chunks):
        low, high = new_kv(chunks, index)
        out_shape += [bf16(BLOCK, (size + 2 * (high - low)) * HEAD_WIDTH)] * peers
    cuts = cut_choices(seq_count)
    plan = in_hbm(owner_plan.T)
    own_query, *packed = pl.pallas_call(
        lambda *refs: pack_kernel(block_axis, dev_width, kv_width, chunks, *refs),
        out_shape=out_shape,
        in_specs=[hbm] * 3,
        out_specs=[vmem] * len(out_shape),
        scratch_shapes=[
            pltpu.SemaphoreType.DMA((1 + 2 * block_axis + 3 * peers * len(chunks),))
        ],
        compiler_params=pltpu.CompilerParams(vmem_limit_bytes=8 << 20),
        name="pack",
    )(*map(in_hbm, (queries, rotated_keys, head_value_rows)))

    sideways = lambda shift: lambda z, x: (z, (x + shift) % block_axis)
    onward = lambda shift: lambda z, x: ((z + 1) % seq_count, (x + shift) % block_axis)
    home = [
        [permute(packed[block_axis + c * peers + s - 1], sideways(s)) for s in range(1, block_axis)]
        for c in range(len(chunks))
    ]
    prior = [permute(packed[s], onward(s)) for s in range(block_axis)]

    results = []
    for index, chunk in enumerate(chunks):
        first, heads = chunk
        width = heads * HEAD_WIDTH
        kv_low, kv_high = kv_range(chunk)
        kv_span = (kv_high - kv_low) * HEAD_WIDTH
        choices = [] if index else [jax.ShapeDtypeStruct((1,), jnp.int32)]
        inputs = [own_query, packed[0], *prior, *sum(home[: index + 1], [])]
        attend = pl.pallas_call(
            lambda *refs, index=index: attend_kernel(
                seq_count, block_axis, pair_room, kv_width, chunks, cuts, index, *refs
            ),
            out_shape=[bf16(slot_rows, width)] * seq_count + choices,
            in_specs=[smem, smem] + [vmem] * len(inputs),
            out_specs=[vmem] * seq_count + [smem] * len(choices),
            scratch_shapes=[
                pltpu.VMEM((block_axis, heads * BLOCK, HEAD_WIDTH), jnp.bfloat16),
                pltpu.VMEM((2 * block_axis * BLOCK, kv_span), jnp.bfloat16),
                pltpu.VMEM((2 * block_axis * BLOCK, kv_span), jnp.bfloat16),
            ],
            cost_estimate=pl.CostEstimate(
                flops=8 * group_blocks * BLOCK * window * width,
                bytes_accessed=2 * seq_count * slot_rows * width,
                transcendentals=group_blocks * BLOCK * window * heads,
            ),
            compiler_params=pltpu.CompilerParams(vmem_limit_bytes=16 << 20),
        )
        messages = attend(in_hbm(doc_lengths), plan, *inputs)
        if index == 0:
            messages, (choice,) = messages[:-1], messages[-1:]
        results.append(messages)

    def deliver(left_out, messages):
        def target(step, z, x):
            owner = owner_of(step, z, x, seq_count, block_axis)
            return None if (z, owner) in left_out else (owner, z // per_owner)

        return [
            permute(message, lambda z, x: target(step, z, x))
            for step, message in enumerate(messages)
        ]

    def place(index, arrived, *carried):
        return pl.pallas_call(
            lambda *refs: place_kernel(seq_count, block_axis, dev_width, chunks[index][0], *refs),
            out_shape=bf16(per_owner * slot_rows, heads_tp * HEAD_WIDTH),
            in_specs=[vmem] * seq_count + [anywhere] * len(carried),
            out_specs=anywhere,
            scratch_shapes=[pltpu.SemaphoreType.DMA((seq_count,))],
            input_output_aliases={seq_count: 0} if carried else {},
            compiler_params=pltpu.CompilerParams(vmem_limit_bytes=8 << 20),
        )(*arrived, *carried)

    last = len(chunks) - 1
    arrived = [deliver((), results[index]) for index in range(last)]
    if cuts:
        branches = [
            lambda *messages, cut=cut: place(last, deliver(cut, messages))
            for cut in [*cuts, ()]
        ]
        out = lax.switch(choice[0], branches, *results[last])
    else:
        out = place(last, deliver((), results[last]))
    for index in range(last):
        out = place(index, arrived[index], out)
    return out


def solution(mesh):
    in_specs = (
        P(("groups", "seq", "blk"), "tp"),
        P(("groups", "seq", "blk"), "tp"),
        P(("groups", "seq", "blk"), "tp"),
        P("groups"),
        P("groups", None),
    )
    out_specs = P(("groups", "seq", "blk"), "tp")

    return jax.shard_map(
        per_device, mesh=mesh, in_specs=in_specs, out_specs=out_specs, check_vma=False
    )
```

```python
import math

import jax
import jax.numpy as jnp
from jax import lax
from jax.experimental import pallas as pl
from jax.experimental.pallas import tpu as pltpu
from jax.sharding import PartitionSpec as P


QUERY_HEADS = 64
KEY_HEADS = 8
HEAD_WIDTH = 128
BLOCK = 128
HEADS_PER_GROUP = QUERY_HEADS // KEY_HEADS


masked_score = -1e30
exponent_scale = math.log2(math.e) / math.sqrt(HEAD_WIDTH)
vmem = pl.BlockSpec(memory_space=pltpu.VMEM)
smem = pl.BlockSpec(memory_space=pltpu.SMEM)
anywhere = pl.BlockSpec(memory_space=pl.ANY)
hbm = pl.BlockSpec(memory_space=pltpu.HBM)


def owner_of(step, group, blk, seq_count, block_axis):
    per_owner = seq_count // block_axis
    return (step + blk * per_owner + group % per_owner) % seq_count


def in_hbm(array):
    return pltpu.with_memory_space_constraint(array, pltpu.HBM)


def lanes(first, size):
    return pl.ds(pl.multiple_of(first, HEAD_WIDTH), size)


def kv_first(blk, dev_width):
    return blk * dev_width // (HEAD_WIDTH * HEADS_PER_GROUP) * HEAD_WIDTH


def kv_range(chunk):
    first, heads = chunk
    return first // HEADS_PER_GROUP, (first + heads - 1) // HEADS_PER_GROUP + 1


def new_kv(chunks, index):
    seen = kv_range(chunks[index - 1])[1] if index else 0
    return seen, kv_range(chunks[index])[1]


def cut_choices(seq_count):
    if seq_count != 4:
        return []
    half = seq_count // 2
    low, high = range(half), range(half, seq_count)
    up = [(group, owner) for group in low for owner in high]
    down = [(group, owner) for group in high for owner in low]
    order = ((0, 1), (0, 2), (0, 3), (1, 2), (1, 3), (2, 0), (2, 3), (3, 0), (3, 1))
    return [(up[u], down[d]) for u, d in order]


def is_empty(plan_ref, pair_room, pair):
    group, owner = pair
    empty = jnp.bool_(True)
    for block in range(plan_ref.shape[0]):
        slot = plan_ref[block, group]
        empty = empty & ((slot < owner * pair_room) | (slot >= (owner + 1) * pair_room))
    return empty


def pack_kernel(block_axis, dev_width, kv_width, chunks, query_ref, key_ref, value_ref, *refs):
    refs = list(refs)
    blk = lax.axis_index("blk")
    sems = refs.pop()
    moves = []

    def move_kv(target_ref, to, low, high):
        span = (high - low) * HEAD_WIDTH
        kv = lanes(kv_first(to, dev_width) + low * HEAD_WIDTH, span)
        for index, source_ref in enumerate((key_ref, value_ref)):
            moves.append((source_ref.at[:, kv], target_ref.at[:, pl.ds(index * span, span)]))

    def move_query(target_ref, to, first, size, at):
        columns = lanes(to * dev_width + first * HEAD_WIDTH, size * HEAD_WIDTH)
        target = target_ref.at[:, pl.ds(at, size * HEAD_WIDTH)]
        moves.append((query_ref.at[:, columns], target))

    move_query(refs.pop(0), blk, 0, dev_width // HEAD_WIDTH, 0)
    move_kv(refs.pop(0), blk, 0, kv_width // HEAD_WIDTH)
    for index, (first, size) in enumerate(chunks):
        low, high = new_kv(chunks, index)
        for shift in range(1, block_axis):
            to = lax.rem(blk + shift, block_axis)
            home_ref = refs.pop(0)
            if high > low:
                move_kv(home_ref, to, low, high)
                move_kv(refs.pop(0), to, low, high)
            move_query(home_ref, to, first, size, 2 * (high - low) * HEAD_WIDTH)
    copies = [
        pltpu.make_async_copy(source, target, sems.at[index])
        for index, (source, target) in enumerate(moves)
    ]
    for copy in copies:
        copy.start()
    for copy in copies:
        copy.wait()


def prepare_kernel(block_axis, pair_room, cuts, doc_ref, plan_ref, start_ref, choice_ref):
    group = lax.axis_index("seq")
    first_row = group * block_axis * BLOCK
    row_pos = first_row + lax.broadcasted_iota(jnp.int32, start_ref.shape, 0)

    def reach(index, carried):
        end, start = carried
        end = end + doc_ref[index]
        return end, jnp.where(row_pos >= end, end, start)

    _, start = lax.fori_loop(
        0, doc_ref.shape[0], reach, (jnp.int32(0), jnp.zeros(start_ref.shape, jnp.int32))
    )
    start_ref[...] = start
    empty = {}
    for pair in sum(cuts, ()):
        if pair not in empty:
            empty[pair] = is_empty(plan_ref, pair_room, pair)
    choice = jnp.int32(len(cuts))
    for number, (up, down) in reversed(list(enumerate(cuts))):
        choice = jnp.where(empty[up] & empty[down], number, choice)
    choice_ref[0] = choice


def attend_kernel(seq_count, block_axis, pair_room, kv_width, chunks, index, *refs):
    refs = list(refs)
    take = lambda count: [refs.pop(0) for _ in range(count)]
    plan_ref, start_ref, own_query, own_kv, straight = take(5)
    home_refs, cross_refs = [], []
    for came in range(index + 1):
        low, high = new_kv(chunks, came)
        home_refs.append(take(block_axis - 1))
        cross_refs.append(take(block_axis - 1 if high > low else 0))
    message_refs = take(seq_count)
    query_all, key_all, value_all, result = refs
    group = lax.axis_index("seq")
    blk = lax.axis_index("blk")
    group_len = block_axis * BLOCK
    window = group_len + BLOCK
    first, heads = chunks[index]
    columns = heads * HEAD_WIDTH
    kv_low, kv_high = kv_range(chunks[index])
    kv_from, kv_to = kv_low * HEAD_WIDTH, kv_high * HEAD_WIDTH
    new_low, new_high = new_kv(chunks, index)
    query_at = 2 * (new_high - new_low) * HEAD_WIDTH

    for shift in range(block_axis):
        origin = lax.rem(blk - shift + block_axis, block_axis)
        rows = pl.ds(pl.multiple_of(origin * BLOCK, BLOCK), BLOCK)
        near_rows = pl.ds(pl.multiple_of(group_len + origin * BLOCK, BLOCK), BLOCK)
        if shift == 0:
            query = own_query[:, first * HEAD_WIDTH : first * HEAD_WIDTH + columns]
            for to_rows, source in ((near_rows, own_kv), (rows, straight)):
                key_all[to_rows, :] = source[:, kv_from:kv_to]
                value_all[to_rows, :] = source[:, kv_width + kv_from : kv_width + kv_to]
        else:
            query = home_refs[index][shift - 1][:, query_at : query_at + columns]
            for came in range(index + 1):
                low, high = new_kv(chunks, came)
                span = (high - low) * HEAD_WIDTH
                skip = max(kv_low - low, 0) * HEAD_WIDTH
                if skip >= span:
                    continue
                to = slice((low - kv_low) * HEAD_WIDTH + skip, (high - kv_low) * HEAD_WIDTH)
                for to_rows, sources in ((near_rows, home_refs), (rows, cross_refs)):
                    source = sources[came][shift - 1]
                    key_all[to_rows, to] = source[:, skip:span]
                    value_all[to_rows, to] = source[:, span + skip : 2 * span]
        for head in range(heads):
            query_all[origin, head * BLOCK : (head + 1) * BLOCK, :] = query[
                :, head * HEAD_WIDTH : (head + 1) * HEAD_WIDTH
            ]

    def attend(block, carried):
        first_row = group * group_len + block * BLOCK
        query_pos = first_row + lax.broadcasted_iota(jnp.int32, (BLOCK, window), 0)
        key_pos = first_row - group_len + lax.broadcasted_iota(jnp.int32, (BLOCK, window), 1)
        query_rows = pl.ds(pl.multiple_of(block * BLOCK, BLOCK), BLOCK)
        key_rows = pl.ds(pl.multiple_of(block * BLOCK, BLOCK), window)
        start = jnp.concatenate([start_ref[query_rows, :]] * (window // HEAD_WIDTH), axis=1)
        allowed = (key_pos >= start) & (key_pos <= query_pos)
        for kv in range(kv_low, kv_high):
            low = max(first, kv * HEADS_PER_GROUP) - first
            high = min(first + heads, (kv + 1) * HEADS_PER_GROUP) - first
            kv_at = slice((kv - kv_low) * HEAD_WIDTH, (kv - kv_low + 1) * HEAD_WIDTH)
            scores = lax.dot_general(
                query_all[block, low * BLOCK : high * BLOCK, :],
                key_all[key_rows, kv_at],
                (((1,), (1,)), ((), ())),
                preferred_element_type=jnp.float32,
            )
            weights, totals = [], []
            for head in range(high - low):
                score = scores[head * BLOCK : (head + 1) * BLOCK]
                score = jnp.where(allowed, score, masked_score)
                top = jnp.max(score, axis=1, keepdims=True)
                weight = jnp.exp2((score - top) * exponent_scale)
                totals.append(jnp.sum(weight, axis=1, keepdims=True))
                weights.append(weight.astype(jnp.bfloat16))
            mixed = jnp.dot(
                jnp.concatenate(weights, axis=0),
                value_all[key_rows, kv_at],
                preferred_element_type=jnp.float32,
            )
            for head in range(high - low):
                at = slice((low + head) * HEAD_WIDTH, (low + head + 1) * HEAD_WIDTH)
                result[block, :, at] = (
                    mixed[head * BLOCK : (head + 1) * BLOCK] / totals[head]
                ).astype(jnp.bfloat16)
        return carried

    lax.fori_loop(0, block_axis, attend, 0)

    for step in range(seq_count):
        owner = owner_of(step, group, blk, seq_count, block_axis)
        for pair in range(pair_room):
            chosen = jnp.int32(-1)
            for block in range(plan_ref.shape[0]):
                chosen = jnp.where(
                    plan_ref[block, group] == owner * pair_room + pair, block, chosen
                )
            out_rows = slice(pair * BLOCK, (pair + 1) * BLOCK)

            @pl.when(chosen >= 0)
            def _():
                message_refs[step][out_rows, :] = result[chosen]

            @pl.when(chosen < 0)
            def _():
                message_refs[step][out_rows, :] = jnp.zeros((BLOCK, columns), jnp.bfloat16)


def place_kernel(seq_count, block_axis, places, *refs):
    *sources, out_ref, sems = refs
    group = lax.axis_index("seq")
    per_owner = seq_count // block_axis
    moves = []
    for first, stride in places:
        if len(sources) == 1:
            (whole,) = sources
            width = whole.shape[1] // block_axis
            for blk in range(block_axis):
                target = out_ref.at[:, pl.ds(first + blk * stride, width)]
                moves.append((whole.at[:, pl.ds(blk * width, width)], target))
            break
        for step in range(seq_count):
            message_ref = sources.pop(0)
            rows, width = message_ref.shape
            origin = lax.rem(group - step + seq_count, seq_count)
            at_rows = pl.ds(pl.multiple_of(lax.rem(origin, per_owner) * rows, rows), rows)
            at_lanes = lanes(first + origin // per_owner * stride, width)
            moves.append((message_ref, out_ref.at[at_rows, at_lanes]))
    copies = [
        pltpu.make_async_copy(source, target, sems.at[index])
        for index, (source, target) in enumerate(moves)
    ]
    for copy in copies:
        copy.start()
    for copy in copies:
        copy.wait()


def per_device(queries, rotated_keys, head_value_rows, doc_lengths, owner_plan):
    block_axis = lax.axis_size("blk")
    seq_count = lax.axis_size("seq")
    local_tokens = queries.shape[0]
    group_blocks = local_tokens * block_axis // BLOCK
    heads_tp = queries.shape[1] // HEAD_WIDTH
    heads_dev = heads_tp // block_axis
    groups_kv = max(1, heads_dev // HEADS_PER_GROUP)
    dev_width = heads_dev * HEAD_WIDTH
    kv_width = groups_kv * HEAD_WIDTH
    pair_room = -(-2 * group_blocks // seq_count)
    per_owner = seq_count // block_axis
    slot_rows = pair_room * BLOCK
    window = (block_axis + 1) * BLOCK
    assert local_tokens == BLOCK and seq_count % block_axis == 0

    def permute(array, target):
        pairs = []
        for z in range(seq_count):
            for x in range(block_axis):
                to = target(z, x)
                if to is not None:
                    pairs.append((z * block_axis + x, to[0] * block_axis + to[1]))
        return lax.ppermute(array, ("seq", "blk"), pairs)

    early = heads_dev * 5 // 16
    head_counts = [early, heads_dev - early]
    chunks = [(sum(head_counts[:i]), count) for i, count in enumerate(head_counts)]
    cuts = cut_choices(seq_count)
    plan = in_hbm(owner_plan.T)
    peers = block_axis - 1

    bf16 = lambda *shape: jax.ShapeDtypeStruct(shape, jnp.bfloat16)
    entries = [("own_query", dev_width), ("own_kv", 2 * kv_width)]
    for index, (first, size) in enumerate(chunks):
        low, high = new_kv(chunks, index)
        span = 2 * (high - low) * HEAD_WIDTH
        for _ in range(1, block_axis):
            entries.append((f"home_{index}", span + size * HEAD_WIDTH))
            if span:
                entries.append((f"cross_{index}", span))
    packed = pl.pallas_call(
        lambda *refs: pack_kernel(block_axis, dev_width, kv_width, chunks, *refs),
        out_shape=[bf16(BLOCK, width) for _, width in entries],
        in_specs=[hbm] * 3,
        out_specs=[vmem] * len(entries),
        scratch_shapes=[pltpu.SemaphoreType.DMA((3 + 5 * peers * len(chunks),))],
        compiler_params=pltpu.CompilerParams(vmem_limit_bytes=8 << 20),
        name="pack",
    )(*map(in_hbm, (queries, rotated_keys, head_value_rows)))
    named = lambda name: [array for (entry, _), array in zip(entries, packed) if entry == name]
    (own_query,), (own_kv,) = named("own_query"), named("own_kv")

    prepare = pl.pallas_call(
        lambda *refs: prepare_kernel(block_axis, pair_room, cuts, *refs),
        out_shape=[
            jax.ShapeDtypeStruct((block_axis * BLOCK, HEAD_WIDTH), jnp.int32),
            jax.ShapeDtypeStruct((1,), jnp.int32),
        ],
        in_specs=[smem, smem],
        out_specs=[vmem, smem],
        compiler_params=pltpu.CompilerParams(vmem_limit_bytes=8 << 20),
        name="prepare",
    )
    start, choice = prepare(in_hbm(doc_lengths), plan)

    def exchange(index):
        home = [
            permute(array, lambda z, x: (z, (x + shift) % block_axis))
            for shift, array in enumerate(named(f"home_{index}"), 1)
        ]
        return home

    def onward(array, shift):
        return permute(array, lambda z, x: ((z + 1) % seq_count, (x + shift) % block_axis))

    straight = onward(own_kv, 0)
    cross = [
        [onward(array, shift) for shift, array in enumerate(named(f"cross_{index}"), 1)]
        for index in range(len(chunks))
    ]

    def attend(index, homes):
        heads = chunks[index][1]
        width = heads * HEAD_WIDTH
        kv_low, kv_high = kv_range(chunks[index])
        kv_span = (kv_high - kv_low) * HEAD_WIDTH
        inputs = [start, own_query, own_kv, straight]
        for home, crossed in zip(homes, cross):
            inputs += [*home, *crossed]
        return pl.pallas_call(
            lambda *refs: attend_kernel(
                seq_count, block_axis, pair_room, kv_width, chunks, index, *refs
            ),
            out_shape=[bf16(slot_rows, width)] * seq_count,
            in_specs=[smem] + [vmem] * len(inputs),
            out_specs=[vmem] * seq_count,
            scratch_shapes=[
                pltpu.VMEM((block_axis, heads * BLOCK, HEAD_WIDTH), jnp.bfloat16),
                pltpu.VMEM((2 * block_axis * BLOCK, kv_span), jnp.bfloat16),
                pltpu.VMEM((2 * block_axis * BLOCK, kv_span), jnp.bfloat16),
                pltpu.VMEM((block_axis, BLOCK, width), jnp.bfloat16),
            ],
            cost_estimate=pl.CostEstimate(
                flops=8 * group_blocks * BLOCK * window * width,
                bytes_accessed=2 * seq_count * slot_rows * width,
                transcendentals=group_blocks * BLOCK * window * heads,
            ),
            compiler_params=pltpu.CompilerParams(vmem_limit_bytes=16 << 20),
        )(plan, *inputs)

    def deliver(left_out, messages):
        def target(step, z, x):
            owner = owner_of(step, z, x, seq_count, block_axis)
            return None if (z, owner) in left_out else (owner, z // per_owner)

        return [
            permute(message, lambda z, x: target(step, z, x))
            for step, message in enumerate(messages)
        ]

    homes = [exchange(index) for index in range(len(chunks))]
    results = [attend(index, homes[: index + 1]) for index in range(len(chunks))]
    last = len(chunks) - 1
    arrived = [deliver((), results[index]) for index in range(last)]
    last_width = chunks[last][1] * HEAD_WIDTH
    rows = per_owner * slot_rows

    def gather(left_out, messages):
        return pl.pallas_call(
            lambda *refs: place_kernel(seq_count, block_axis, [(0, last_width)], *refs),
            out_shape=bf16(rows, block_axis * last_width),
            in_specs=[vmem] * seq_count,
            out_specs=anywhere,
            scratch_shapes=[pltpu.SemaphoreType.DMA((seq_count,))],
            compiler_params=pltpu.CompilerParams(vmem_limit_bytes=8 << 20),
            name="gather",
        )(*deliver(left_out, messages))

    if cuts:
        branches = [lambda *messages, cut=cut: gather(cut, messages) for cut in [*cuts, ()]]
        gathered = lax.switch(choice[0], branches, *results[last])
    else:
        gathered = gather((), results[last])
    places = [(first * HEAD_WIDTH, dev_width) for first, _ in chunks]
    return pl.pallas_call(
        lambda *refs: place_kernel(seq_count, block_axis, places, *refs),
        out_shape=bf16(rows, heads_tp * HEAD_WIDTH),
        in_specs=[vmem] * (seq_count * last + 1),
        out_specs=hbm,
        scratch_shapes=[pltpu.SemaphoreType.DMA((seq_count * last + block_axis,))],
        compiler_params=pltpu.CompilerParams(vmem_limit_bytes=8 << 20),
        name="place",
    )(*sum(arrived, []), gathered)


def solution(mesh):
    in_specs = (
        P(("groups", "seq", "blk"), "tp"),
        P(("groups", "seq", "blk"), "tp"),
        P(("groups", "seq", "blk"), "tp"),
        P("groups"),
        P("groups", None),
    )
    out_specs = P(("groups", "seq", "blk"), "tp")

    return jax.shard_map(
        per_device, mesh=mesh, in_specs=in_specs, out_specs=out_specs, check_vma=False
    )
```

```python
import math

import jax
import jax.numpy as jnp
from jax import lax
from jax.experimental import pallas as pl
from jax.experimental.pallas import tpu as pltpu
from jax.sharding import PartitionSpec as P


QUERY_HEADS = 64
KEY_HEADS = 8
HEAD_WIDTH = 128
BLOCK = 128
HEADS_PER_GROUP = QUERY_HEADS // KEY_HEADS


masked_score = -1e30
exponent_scale = math.log2(math.e) / math.sqrt(HEAD_WIDTH)
vmem = pl.BlockSpec(memory_space=pltpu.VMEM)
smem = pl.BlockSpec(memory_space=pltpu.SMEM)
anywhere = pl.BlockSpec(memory_space=pl.ANY)
hbm = pl.BlockSpec(memory_space=pltpu.HBM)


def owner_of(step, group, blk, seq_count, block_axis):
    per_owner = seq_count // block_axis
    return (step + blk * per_owner + group % per_owner) % seq_count


def in_hbm(array):
    return pltpu.with_memory_space_constraint(array, pltpu.HBM)


def lanes(first, size):
    return pl.ds(pl.multiple_of(first, HEAD_WIDTH), size)


def kv_first(blk, dev_width):
    return blk * dev_width // (HEAD_WIDTH * HEADS_PER_GROUP) * HEAD_WIDTH


def kv_range(chunk):
    first, heads = chunk
    return first // HEADS_PER_GROUP, (first + heads - 1) // HEADS_PER_GROUP + 1


def new_kv(chunks, index):
    seen = kv_range(chunks[index - 1])[1] if index else 0
    return seen, kv_range(chunks[index])[1]


def cut_choices(seq_count):
    if seq_count != 4:
        return []
    half = seq_count // 2
    low, high = range(half), range(half, seq_count)
    up = [(group, owner) for group in low for owner in high]
    down = [(group, owner) for group in high for owner in low]
    order = ((1, 2), (3, 0), (3, 2), (0, 3), (0, 2), (1, 0), (2, 2), (1, 3), (2, 1))
    return [(up[u], down[d]) for u, d in order]


def is_empty(plan_ref, pair_room, pair):
    group, owner = pair
    empty = jnp.bool_(True)
    for block in range(plan_ref.shape[0]):
        slot = plan_ref[block, group]
        empty = empty & ((slot < owner * pair_room) | (slot >= (owner + 1) * pair_room))
    return empty


def pack_kernel(block_axis, dev_width, kv_width, chunks, query_ref, key_ref, value_ref, *refs):
    refs = list(refs)
    blk = lax.axis_index("blk")
    sems = refs.pop()
    moves = []

    def move_kv(target_ref, to, low, high):
        span = (high - low) * HEAD_WIDTH
        kv = lanes(kv_first(to, dev_width) + low * HEAD_WIDTH, span)
        for index, source_ref in enumerate((key_ref, value_ref)):
            moves.append((source_ref.at[:, kv], target_ref.at[:, pl.ds(index * span, span)]))

    def move_query(target_ref, to, first, size, at):
        columns = lanes(to * dev_width + first * HEAD_WIDTH, size * HEAD_WIDTH)
        target = target_ref.at[:, pl.ds(at, size * HEAD_WIDTH)]
        moves.append((query_ref.at[:, columns], target))

    move_query(refs.pop(0), blk, 0, dev_width // HEAD_WIDTH, 0)
    move_kv(refs.pop(0), blk, 0, kv_width // HEAD_WIDTH)
    for index, (first, size) in enumerate(chunks):
        low, high = new_kv(chunks, index)
        for shift in range(1, block_axis):
            to = lax.rem(blk + shift, block_axis)
            home_ref = refs.pop(0)
            if high > low:
                move_kv(home_ref, to, low, high)
                move_kv(refs.pop(0), to, low, high)
            move_query(home_ref, to, first, size, 2 * (high - low) * HEAD_WIDTH)
    copies = [
        pltpu.make_async_copy(source, target, sems.at[index])
        for index, (source, target) in enumerate(moves)
    ]
    for copy in copies:
        copy.start()
    for copy in copies:
        copy.wait()


def prepare_kernel(block_axis, pair_room, cuts, doc_ref, plan_ref, start_ref, choice_ref):
    group = lax.axis_index("seq")
    first_row = group * block_axis * BLOCK
    row_pos = first_row + lax.broadcasted_iota(jnp.int32, start_ref.shape, 0)

    def reach(index, carried):
        end, start = carried
        end = end + doc_ref[index]
        return end, jnp.where(row_pos >= end, end, start)

    _, start = lax.fori_loop(
        0, doc_ref.shape[0], reach, (jnp.int32(0), jnp.zeros(start_ref.shape, jnp.int32))
    )
    start_ref[...] = start
    empty = {}
    for pair in sum(cuts, ()):
        if pair not in empty:
            empty[pair] = is_empty(plan_ref, pair_room, pair)
    choice = jnp.int32(len(cuts))
    for number, (up, down) in reversed(list(enumerate(cuts))):
        choice = jnp.where(empty[up] & empty[down], number, choice)
    choice_ref[0] = choice


def attend_kernel(seq_count, block_axis, pair_room, kv_width, chunks, index, *refs):
    refs = list(refs)
    take = lambda count: [refs.pop(0) for _ in range(count)]
    plan_hbm, start_ref, own_query, own_kv, straight = take(5)
    home_refs, cross_refs = [], []
    for came in range(index + 1):
        low, high = new_kv(chunks, came)
        home_refs.append(take(block_axis - 1))
        cross_refs.append(take(block_axis - 1 if high > low else 0))
    message_refs = take(seq_count)
    query_all, key_all, value_all, result, plan_ref, plan_sem = refs
    plan_copy = pltpu.make_async_copy(plan_hbm, plan_ref, plan_sem)
    plan_copy.start()
    group = lax.axis_index("seq")
    blk = lax.axis_index("blk")
    group_len = block_axis * BLOCK
    window = group_len + BLOCK
    first, heads = chunks[index]
    columns = heads * HEAD_WIDTH
    kv_low, kv_high = kv_range(chunks[index])
    kv_from, kv_to = kv_low * HEAD_WIDTH, kv_high * HEAD_WIDTH
    new_low, new_high = new_kv(chunks, index)
    query_at = 2 * (new_high - new_low) * HEAD_WIDTH

    for shift in range(block_axis):
        origin = lax.rem(blk - shift + block_axis, block_axis)
        rows = pl.ds(pl.multiple_of(origin * BLOCK, BLOCK), BLOCK)
        near_rows = pl.ds(pl.multiple_of(group_len + origin * BLOCK, BLOCK), BLOCK)
        if shift == 0:
            query = own_query[:, first * HEAD_WIDTH : first * HEAD_WIDTH + columns]
            for to_rows, source in ((near_rows, own_kv), (rows, straight)):
                key_all[to_rows, :] = source[:, kv_from:kv_to]
                value_all[to_rows, :] = source[:, kv_width + kv_from : kv_width + kv_to]
        else:
            query = home_refs[index][shift - 1][:, query_at : query_at + columns]
            for came in range(index + 1):
                low, high = new_kv(chunks, came)
                span = (high - low) * HEAD_WIDTH
                skip = max(kv_low - low, 0) * HEAD_WIDTH
                if skip >= span:
                    continue
                to = slice((low - kv_low) * HEAD_WIDTH + skip, (high - kv_low) * HEAD_WIDTH)
                for to_rows, sources in ((near_rows, home_refs), (rows, cross_refs)):
                    source = sources[came][shift - 1]
                    key_all[to_rows, to] = source[:, skip:span]
                    value_all[to_rows, to] = source[:, span + skip : 2 * span]
        for head in range(heads):
            query_all[origin, head * BLOCK : (head + 1) * BLOCK, :] = query[
                :, head * HEAD_WIDTH : (head + 1) * HEAD_WIDTH
            ]

    def attend(block, carried):
        first_row = group * group_len + block * BLOCK
        query_pos = first_row + lax.broadcasted_iota(jnp.int32, (BLOCK, window), 0)
        key_pos = first_row - group_len + lax.broadcasted_iota(jnp.int32, (BLOCK, window), 1)
        query_rows = pl.ds(pl.multiple_of(block * BLOCK, BLOCK), BLOCK)
        key_rows = pl.ds(pl.multiple_of(block * BLOCK, BLOCK), window)
        start = jnp.concatenate([start_ref[query_rows, :]] * (window // HEAD_WIDTH), axis=1)
        allowed = (key_pos >= start) & (key_pos <= query_pos)
        for kv in range(kv_low, kv_high):
            low = max(first, kv * HEADS_PER_GROUP) - first
            high = min(first + heads, (kv + 1) * HEADS_PER_GROUP) - first
            kv_at = slice((kv - kv_low) * HEAD_WIDTH, (kv - kv_low + 1) * HEAD_WIDTH)
            scores = lax.dot_general(
                query_all[block, low * BLOCK : high * BLOCK, :],
                key_all[key_rows, kv_at],
                (((1,), (1,)), ((), ())),
                preferred_element_type=jnp.float32,
            )
            weights, totals = [], []
            for head in range(high - low):
                score = scores[head * BLOCK : (head + 1) * BLOCK]
                score = jnp.where(allowed, score, masked_score)
                top = jnp.max(score, axis=1, keepdims=True)
                weight = jnp.exp2((score - top) * exponent_scale)
                totals.append(jnp.sum(weight, axis=1, keepdims=True))
                weights.append(weight.astype(jnp.bfloat16))
            mixed = jnp.dot(
                jnp.concatenate(weights, axis=0),
                value_all[key_rows, kv_at],
                preferred_element_type=jnp.float32,
            )
            for head in range(high - low):
                at = slice((low + head) * HEAD_WIDTH, (low + head + 1) * HEAD_WIDTH)
                result[block, :, at] = (
                    mixed[head * BLOCK : (head + 1) * BLOCK] / totals[head]
                ).astype(jnp.bfloat16)
        return carried

    lax.fori_loop(0, block_axis, attend, 0)
    plan_copy.wait()

    for step in range(seq_count):
        owner = owner_of(step, group, blk, seq_count, block_axis)
        for pair in range(pair_room):
            chosen = jnp.int32(-1)
            for block in range(plan_ref.shape[0]):
                chosen = jnp.where(
                    plan_ref[block, group] == owner * pair_room + pair, block, chosen
                )
            out_rows = slice(pair * BLOCK, (pair + 1) * BLOCK)

            @pl.when(chosen >= 0)
            def _():
                message_refs[step][out_rows, :] = result[chosen]

            @pl.when(chosen < 0)
            def _():
                message_refs[step][out_rows, :] = jnp.zeros((BLOCK, columns), jnp.bfloat16)


def place_kernel(seq_count, block_axis, places, *refs):
    *sources, out_ref, sems = refs
    group = lax.axis_index("seq")
    per_owner = seq_count // block_axis
    moves = []
    for first, stride in places:
        if len(sources) == 1:
            (whole,) = sources
            width = whole.shape[1] // block_axis
            for blk in range(block_axis):
                target = out_ref.at[:, pl.ds(first + blk * stride, width)]
                moves.append((whole.at[:, pl.ds(blk * width, width)], target))
            break
        for step in range(seq_count):
            message_ref = sources.pop(0)
            rows, width = message_ref.shape
            origin = lax.rem(group - step + seq_count, seq_count)
            at_rows = pl.ds(pl.multiple_of(lax.rem(origin, per_owner) * rows, rows), rows)
            at_lanes = lanes(first + origin // per_owner * stride, width)
            moves.append((message_ref, out_ref.at[at_rows, at_lanes]))
    copies = [
        pltpu.make_async_copy(source, target, sems.at[index])
        for index, (source, target) in enumerate(moves)
    ]
    for copy in copies:
        copy.start()
    for copy in copies:
        copy.wait()


def per_device(queries, rotated_keys, head_value_rows, doc_lengths, owner_plan):
    block_axis = lax.axis_size("blk")
    seq_count = lax.axis_size("seq")
    local_tokens = queries.shape[0]
    group_blocks = local_tokens * block_axis // BLOCK
    heads_tp = queries.shape[1] // HEAD_WIDTH
    heads_dev = heads_tp // block_axis
    groups_kv = max(1, heads_dev // HEADS_PER_GROUP)
    dev_width = heads_dev * HEAD_WIDTH
    kv_width = groups_kv * HEAD_WIDTH
    pair_room = -(-2 * group_blocks // seq_count)
    per_owner = seq_count // block_axis
    slot_rows = pair_room * BLOCK
    window = (block_axis + 1) * BLOCK
    assert local_tokens == BLOCK and seq_count % block_axis == 0

    def permute(array, target):
        pairs = []
        for z in range(seq_count):
            for x in range(block_axis):
                to = target(z, x)
                if to is not None:
                    pairs.append((z * block_axis + x, to[0] * block_axis + to[1]))
        return lax.ppermute(array, ("seq", "blk"), pairs)

    early = heads_dev * 5 // 16
    head_counts = [early, heads_dev - early]
    chunks = [(sum(head_counts[:i]), count) for i, count in enumerate(head_counts)]
    cuts = cut_choices(seq_count)
    plan = in_hbm(owner_plan.T)
    peers = block_axis - 1

    bf16 = lambda *shape: jax.ShapeDtypeStruct(shape, jnp.bfloat16)
    entries = [("own_query", dev_width), ("own_kv", 2 * kv_width)]
    for index, (first, size) in enumerate(chunks):
        low, high = new_kv(chunks, index)
        span = 2 * (high - low) * HEAD_WIDTH
        for _ in range(1, block_axis):
            entries.append((f"home_{index}", span + size * HEAD_WIDTH))
            if span:
                entries.append((f"cross_{index}", span))
    packed = pl.pallas_call(
        lambda *refs: pack_kernel(block_axis, dev_width, kv_width, chunks, *refs),
        out_shape=[bf16(BLOCK, width) for _, width in entries],
        in_specs=[hbm] * 3,
        out_specs=[vmem] * len(entries),
        scratch_shapes=[pltpu.SemaphoreType.DMA((3 + 5 * peers * len(chunks),))],
        compiler_params=pltpu.CompilerParams(vmem_limit_bytes=8 << 20),
        name="pack",
    )(*map(in_hbm, (queries, rotated_keys, head_value_rows)))
    named = lambda name: [array for (entry, _), array in zip(entries, packed) if entry == name]
    (own_query,), (own_kv,) = named("own_query"), named("own_kv")

    prepare = pl.pallas_call(
        lambda *refs: prepare_kernel(block_axis, pair_room, cuts, *refs),
        out_shape=[
            jax.ShapeDtypeStruct((block_axis * BLOCK, HEAD_WIDTH), jnp.int32),
            jax.ShapeDtypeStruct((1,), jnp.int32),
        ],
        in_specs=[smem, smem],
        out_specs=[vmem, smem],
        compiler_params=pltpu.CompilerParams(vmem_limit_bytes=8 << 20),
        name="prepare",
    )
    start, choice = prepare(in_hbm(doc_lengths), plan)

    def exchange(index):
        home = [
            permute(array, lambda z, x: (z, (x + shift) % block_axis))
            for shift, array in enumerate(named(f"home_{index}"), 1)
        ]
        return home

    def onward(array, shift):
        return permute(array, lambda z, x: ((z + 1) % seq_count, (x + shift) % block_axis))

    straight = onward(own_kv, 0)
    cross = [
        [onward(array, shift) for shift, array in enumerate(named(f"cross_{index}"), 1)]
        for index in range(len(chunks))
    ]

    def attend(index, homes):
        heads = chunks[index][1]
        width = heads * HEAD_WIDTH
        kv_low, kv_high = kv_range(chunks[index])
        kv_span = (kv_high - kv_low) * HEAD_WIDTH
        inputs = [start, own_query, own_kv, straight]
        for home, crossed in zip(homes, cross):
            inputs += [*home, *crossed]
        return pl.pallas_call(
            lambda *refs: attend_kernel(
                seq_count, block_axis, pair_room, kv_width, chunks, index, *refs
            ),
            out_shape=[bf16(slot_rows, width)] * seq_count,
            in_specs=[hbm] + [vmem] * len(inputs),
            out_specs=[vmem] * seq_count,
            scratch_shapes=[
                pltpu.VMEM((block_axis, heads * BLOCK, HEAD_WIDTH), jnp.bfloat16),
                pltpu.VMEM((2 * block_axis * BLOCK, kv_span), jnp.bfloat16),
                pltpu.VMEM((2 * block_axis * BLOCK, kv_span), jnp.bfloat16),
                pltpu.VMEM((block_axis, BLOCK, width), jnp.bfloat16),
                pltpu.SMEM(plan.shape, jnp.int32),
                pltpu.SemaphoreType.DMA,
            ],
            cost_estimate=pl.CostEstimate(
                flops=8 * group_blocks * BLOCK * window * width,
                bytes_accessed=2 * seq_count * slot_rows * width,
                transcendentals=group_blocks * BLOCK * window * heads,
            ),
            compiler_params=pltpu.CompilerParams(vmem_limit_bytes=16 << 20),
        )(plan, *inputs)

    def deliver(left_out, messages):
        def target(step, z, x):
            owner = owner_of(step, z, x, seq_count, block_axis)
            return None if (z, owner) in left_out else (owner, z // per_owner)

        return [
            permute(message, lambda z, x: target(step, z, x))
            for step, message in enumerate(messages)
        ]

    homes = [exchange(index) for index in range(len(chunks))]
    results = [attend(index, homes[: index + 1]) for index in range(len(chunks))]
    last = len(chunks) - 1
    arrived = [deliver((), results[index]) for index in range(last)]
    last_width = chunks[last][1] * HEAD_WIDTH
    rows = per_owner * slot_rows

    def gather(left_out, messages):
        return pl.pallas_call(
            lambda *refs: place_kernel(seq_count, block_axis, [(0, last_width)], *refs),
            out_shape=bf16(rows, block_axis * last_width),
            in_specs=[vmem] * seq_count,
            out_specs=anywhere,
            scratch_shapes=[pltpu.SemaphoreType.DMA((seq_count,))],
            compiler_params=pltpu.CompilerParams(vmem_limit_bytes=8 << 20),
            name="gather",
        )(*deliver(left_out, messages))

    if cuts:
        branches = [lambda *messages, cut=cut: gather(cut, messages) for cut in [*cuts, ()]]
        gathered = lax.switch(choice[0], branches, *results[last])
    else:
        gathered = gather((), results[last])
    places = [(first * HEAD_WIDTH, dev_width) for first, _ in chunks]
    return pl.pallas_call(
        lambda *refs: place_kernel(seq_count, block_axis, places, *refs),
        out_shape=bf16(rows, heads_tp * HEAD_WIDTH),
        in_specs=[vmem] * (seq_count * last + 1),
        out_specs=hbm,
        scratch_shapes=[pltpu.SemaphoreType.DMA((seq_count * last + block_axis,))],
        compiler_params=pltpu.CompilerParams(vmem_limit_bytes=8 << 20),
        name="place",
    )(*sum(arrived, []), gathered)


def solution(mesh):
    in_specs = (
        P(("groups", "seq", "blk"), "tp"),
        P(("groups", "seq", "blk"), "tp"),
        P(("groups", "seq", "blk"), "tp"),
        P("groups"),
        P("groups", None),
    )
    out_specs = P(("groups", "seq", "blk"), "tp")

    return jax.shard_map(
        per_device, mesh=mesh, in_specs=in_specs, out_specs=out_specs, check_vma=False
    )
```
